32 devices in a mesh: dp: 16 (over z, y, core), tensor: 2 (over x).
Axes of the slice: x: 2, y: 2, z: 4, core: 2. Of those that a mesh axis runs over, the one named last changes fastest.
Arguments:
- activations: bfloat16 [4096, 27648], P('dp', 'tensor'), may hold values from -6 to 6
- output_gradient: bfloat16 [4096, 5120], P('dp', 'tensor'), may hold values from -6 to 6
- adapter_a: bfloat16 [2, 13824, 128], P('tensor', 'dp'), may hold values from -0.0390625 to 0.0390625
- adapter_b: bfloat16 [128, 5120], P(None, 'tensor'), may hold values from -0.078125 to 0.078125
- log_ratio: float32 [4096], P('dp'), may hold values from -1.5 to 1.5
- lengths: int32 [1, 16], replicated, may hold values from 1 to 256, as said below
- rewards: int32 [1, 16], replicated, may hold values from 0 to 10
Outputs:
- grad_a: float32 [2, 13824, 128], P('tensor', 'dp')
- adapter_b_gradient: float32 [128, 5120], P(None, 'tensor')
- loss: float32 [], replicated
The draws below stay inside these ranges and needn't reach their ends.
Inputs may be any that keep to these rules, and one draw needn't show every extreme that they name: `lengths`: in every group some rollout has length 256.
All inputs are finite; a program needn't handle non-finite values.
Results may differ from the reference program's by a relative error of at most 0.0067.
Values may be sent and summed in bfloat16 or wider, within the bound.
No kernel may reach another device: no remote copies, remote signals or barrier semaphores. Data moves between devices by JAX's collectives and lax.ppermute only.
A program may use at most 64 MiB of HBM per device.

```python
import jax
import jax.numpy as jnp
from jax import lax

D = 5120
FF = 27648
R = 128
ROLLOUTS = 16
MOST = 256
GROUPS = 1
TOKENS = 4096
TP_BLOCKS = 2
FF_TP = 13824


def draw_lengths(key, part):
    first_key, second_key = jax.random.split(jax.random.fold_in(key, 17))
    base = jax.random.randint(first_key, (GROUPS, ROLLOUTS), 1, MOST + 1)
    chosen = jax.random.randint(second_key, (GROUPS, 1), 0, ROLLOUTS)
    column_ids = jnp.arange(ROLLOUTS)[None, :]
    return jnp.where(column_ids == chosen, MOST, base).astype(jnp.int32)


def with_ends(drawn, rng, low, largest):
    shape = drawn.shape
    place = [jax.random.randint(jax.random.fold_in(rng, axis), (), 0, shape[axis]) for axis in range(len(shape))]
    drawn = drawn.at[tuple(place)].set(low)
    longest = shape.index(max(shape))
    place[longest] = (place[longest] + 1) % shape[longest]
    return drawn.at[tuple(place)].set(largest)


def strengthened(result, key, source, target, blocks, factor):
    owner, partner = [(jnp.arange(result.shape[axis_at]) // (result.shape[axis_at] // blocks)).reshape([-1 if axis == axis_at else 1 for axis in range(result.ndim)]) for axis_at in (source, target)]
    chosen = jax.random.permutation(key, blocks)[partner]
    strong = (owner == chosen) | (owner == (partner + blocks // 2) % blocks)
    return jnp.where(strong, factor * result, result)


def levels(stream_key, dims, cuts, low, top_value):
    def one(position, shards_of):
        heights = jax.random.uniform(jax.random.fold_in(jax.random.fold_in(stream_key, 6), position), (shards_of,), jnp.float32, low / len(cuts), top_value / len(cuts))
        return jnp.repeat(jnp.exp(heights), dims[position] // shards_of).reshape((-1,) + (1,) * (len(dims) - position - 1))

    level = one(*cuts[0])
    for cut in cuts[1:]:
        level = level * one(*cut)
    return level


def centred(rng, shape, deviation, limit, cuts=(), kind=jnp.bfloat16):
    level = levels(rng, shape, cuts, -0.22, 0.18) if cuts else 1.0
    values = jax.random.normal(rng, shape, jnp.float32) * deviation * level
    return jnp.minimum(jnp.maximum(values, -limit), limit).astype(kind)


def noise_with(own_key, shape, scale, bound, pieces, heavy, kind=jnp.bfloat16):
    entries = scale * jax.random.normal(own_key, shape, jnp.float32)
    if pieces:
        entries = entries * levels(own_key, shape, pieces, -0.22, 0.18)
    return jnp.clip(strengthened(entries, jax.random.fold_in(own_key, 3), *heavy), -bound, bound).astype(kind)


def setup_inputs(seed: int = 0) -> dict:
    streams_of = jax.random.split(jax.random.key(seed), 8)
    activations = noise_with(streams_of[0], (TOKENS, FF), 1.0, 6.0, ((0, 16), (1, 2)), (0, 1, 16, 2.0))
    output_gradient = centred(streams_of[1], (TOKENS, D), 1.0, 6.0, ((0, 16), (1, 2)))
    adapter_a = centred(streams_of[2], (TP_BLOCKS, FF_TP, R), FF ** -0.5, 0.0390625, ((0, 2), (1, 16)))
    adapter_b = centred(streams_of[3], (R, D), D ** -0.5, 0.078125, ((1, 2),))
    log_ratio = centred(streams_of[4], (TOKENS,), 0.25, 1.5, ((0, 16),), jnp.float32)
    lengths = draw_lengths(jax.random.fold_in(streams_of[7], 71), 0)
    rewards = with_ends(jax.random.randint(streams_of[6], (GROUPS, ROLLOUTS), 0, 11), jax.random.fold_in(streams_of[6], 1), 0, 10).astype(jnp.int32)
    return dict(activations=activations, output_gradient=output_gradient, adapter_a=adapter_a, adapter_b=adapter_b, log_ratio=log_ratio, lengths=lengths, rewards=rewards)


clip_eps = 0.2
adapter_scale_factor = 2.0

def token_terms(length_row, reward_row, log_ratio, offset):
    reward = reward_row.astype(jnp.float32)
    center = jnp.mean(reward)
    spread = jnp.mean((reward - center) * (reward - center))
    advantage = (reward - center) / jnp.sqrt(spread + 1.0)
    ends = jnp.cumsum(length_row).astype(jnp.int32)
    starts = (ends - length_row).astype(jnp.int32)
    slots = jnp.arange(log_ratio.shape[0], dtype=jnp.int32) + offset
    member = ((slots[None, :] >= starts[:, None]) & (slots[None, :] < ends[:, None])).astype(jnp.float32)
    live = lax.optimization_barrier(jnp.sum(member, axis=0))
    token_adv = lax.optimization_barrier(jnp.sum(member * advantage[:, None], axis=0))
    ratio = jnp.exp(log_ratio)
    unclipped = ratio * token_adv
    clipped = jnp.clip(ratio, 1.0 - clip_eps, 1.0 + clip_eps) * token_adv
    token_loss = -jnp.minimum(unclipped, clipped)
    slope = jnp.where(unclipped <= clipped, -unclipped, jnp.zeros_like(unclipped))
    return (live * slope, jnp.sum(live * token_loss), jnp.sum(live))

def reference(activations, output_gradient, adapter_a, adapter_b, log_ratio, lengths, rewards):
    groups = lengths.shape[0]
    offsets = jnp.zeros((groups,), jnp.int32)
    token_coefficient, loss_parts, live_parts = jax.vmap(token_terms)(lengths, rewards, log_ratio.reshape(groups, -1), offsets)
    token_coefficient = token_coefficient.reshape(-1)
    ratio_multiplier = groups / jnp.sum(live_parts)
    a_whole = adapter_a.reshape(-1, adapter_a.shape[2])
    low_rank = jnp.dot(activations, a_whole, preferred_element_type=jnp.float32)
    backward_projection = jnp.dot(output_gradient, adapter_b.T, preferred_element_type=jnp.float32)
    error_rows = (adapter_scale_factor * token_coefficient[:, None] * backward_projection).astype(jnp.bfloat16)
    grad_a = ratio_multiplier * lax.dot_general(activations, error_rows, (((0,), (0,)), ((), ())), preferred_element_type=jnp.float32)
    weighted_error = token_coefficient[:, None] * low_rank
    adapter_b_gradient = ratio_multiplier * adapter_scale_factor * jnp.dot(weighted_error.T, output_gradient.astype(jnp.float32), precision=lax.Precision.HIGHEST)
    loss = ratio_multiplier * jnp.sum(loss_parts)
    return (grad_a.reshape(adapter_a.shape), adapter_b_gradient, loss)
```

```python
import functools

import jax
import jax.numpy as jnp
from jax import lax
from jax.experimental import pallas as pl
from jax.experimental.pallas import tpu as pltpu
from jax.sharding import PartitionSpec as P

clip_eps = 0.2
adapter_scale_factor = 2.0
cores = 2
lanes = 128


def slot_terms(length_row, reward_row, log_ratio, offset):
    reward = reward_row.astype(jnp.float32)
    center = jnp.mean(reward)
    spread = jnp.mean((reward - center) * (reward - center))
    advantage = (reward - center) / jnp.sqrt(spread + 1.0)
    ends = jnp.cumsum(length_row)
    starts = ends - length_row
    slots = jnp.arange(log_ratio.shape[0], dtype=jnp.int32) + offset
    member = ((slots[None, :] >= starts[:, None]) & (slots[None, :] < ends[:, None])).astype(
        jnp.float32
    )
    live = jnp.sum(member, axis=0)
    token_adv = jnp.sum(member * advantage[:, None], axis=0)
    ratio = jnp.exp(log_ratio)
    unclipped = ratio * token_adv
    clipped = jnp.clip(ratio, 1.0 - clip_eps, 1.0 + clip_eps) * token_adv
    token_loss = -jnp.minimum(unclipped, clipped)
    slope = jnp.where(unclipped <= clipped, -unclipped, jnp.zeros_like(unclipped))
    return (live * slope, jnp.sum(live * token_loss))


def own_terms(log_ratio, lengths, rewards):
    tokens = log_ratio.shape[0]
    groups = lengths.shape[0]
    per_group = lax.axis_size("dp") // groups
    position = lax.axis_index("dp")
    group_id = position // per_group
    offset = position % per_group * tokens
    length_row = lax.dynamic_index_in_dim(lengths, group_id, 0, keepdims=False)
    reward_row = lax.dynamic_index_in_dim(rewards, group_id, 0, keepdims=False)
    coefficient, loss = slot_terms(length_row, reward_row, log_ratio, offset)
    live = jnp.sum(jnp.minimum(jnp.sum(lengths, axis=1), per_group * tokens))
    return coefficient, loss, groups / live.astype(jnp.float32)


def general(activations, output_gradient, adapter_a, adapter_b, log_ratio, lengths, rewards):
    coefficient, loss, factor = own_terms(log_ratio, lengths, rewards)
    partial_low = jnp.dot(
        activations,
        lax.all_gather(adapter_a, "dp", axis=1, tiled=True)[0],
        preferred_element_type=jnp.float32,
    )
    partial_back = lax.dot_general(
        output_gradient, adapter_b, (((1,), (1,)), ((), ())), preferred_element_type=jnp.float32
    )
    low_rank, back = lax.psum((partial_low, partial_back), "tensor")
    error_rows = (adapter_scale_factor * coefficient[:, None] * back).astype(jnp.bfloat16)
    grad_b = adapter_scale_factor * jnp.einsum(
        "tr,td->rd",
        coefficient[:, None] * low_rank,
        output_gradient.astype(jnp.float32),
        precision=lax.Precision.HIGHEST,
    )
    grad_a = lax.psum_scatter(
        lax.dot_general(
            activations, error_rows, (((0,), (0,)), ((), ())), preferred_element_type=jnp.float32
        ),
        "dp",
        scatter_dimension=0,
        tiled=True,
    )
    grad_b, loss = lax.psum((grad_b, loss), "dp")
    return ((factor * grad_a)[None], factor * grad_b, factor * loss)


def low_rank_kernel(rounds, pos, acts, *refs):
    count = len(rounds)
    slices = refs[: 4 * count]
    before = refs[4 * count] if len(refs) == 4 * count + 3 else None
    out, whole = refs[-2:]
    step = pl.program_id(0)
    rows = slices[0].shape[0]
    for index in range(count):

        @pl.when(step == index)
        def _():
            for dy in range(2):
                for dk in range(2):
                    at = ((pos[1] ^ dy) * 2 + (pos[2] ^ dk)) * rows
                    whole[pl.ds(pl.multiple_of(at, rows), rows), :] = slices[
                        4 * index + 2 * dy + dk
                    ][...]

    part = jnp.dot(acts[...], whole[...], preferred_element_type=jnp.float32)

    @pl.when(step == 0)
    def _():
        out[...] = part if before is None else part + before[...]

    @pl.when(step > 0)
    def _():
        out[...] += part


def low_rank_part(pos, activations, rounds, slices, before=None):
    tokens = activations.shape[0]
    rows, rank = slices[0].shape
    width = 4 * rows
    first, step = rounds[0], rounds[1] - rounds[0] if len(rounds) > 1 else 0
    whole = lambda i, p: (0, 0)
    extra = () if before is None else (before,)
    return pl.pallas_call(
        functools.partial(low_rank_kernel, rounds),
        grid_spec=pltpu.PrefetchScalarGridSpec(
            num_scalar_prefetch=1,
            grid=(len(rounds),),
            in_specs=[pl.BlockSpec((tokens, width), lambda i, p: (0, p[0] ^ (first + step * i)))]
            + [pl.BlockSpec((rows, rank), whole)] * len(slices)
            + [pl.BlockSpec((tokens, rank), whole)] * len(extra),
            out_specs=pl.BlockSpec((tokens, rank), whole),
            scratch_shapes=[pltpu.VMEM((width, rank), jnp.bfloat16)],
        ),
        out_shape=jax.ShapeDtypeStruct((tokens, rank), jnp.float32),
        cost_estimate=pl.CostEstimate(
            flops=2 * tokens * width * rank * len(rounds),
            bytes_accessed=2 * (tokens + rank) * width * len(rounds),
            transcendentals=0,
        ),
        name="low_rank",
    )(pos, activations, *slices, *extra)


def grad_a_kernel(pos, acts, err, keep, send, whole):
    rows = keep.shape[2]
    whole[...] = lax.dot_general(
        acts[...], err[...], (((0,), (0,)), ((), ())), preferred_element_type=jnp.float32
    )
    for dk, out in enumerate((keep, send)):
        for dy in range(2):
            at = ((pos[1] ^ dy) * 2 + (pos[2] ^ dk)) * rows
            out[dy, 0] = whole[pl.ds(pl.multiple_of(at, rows), rows), :].astype(jnp.bfloat16)


def grad_a_part(pos, activations, err, rounds, rows):
    tokens, rank = err.shape
    width = 4 * rows
    count = len(rounds)
    first, step = rounds[0], rounds[1] - rounds[0] if count > 1 else 0
    spec = pl.BlockSpec((2, 1, rows, rank), lambda i, p: (0, i, 0, 0))
    shape = jax.ShapeDtypeStruct((2, count, rows, rank), jnp.bfloat16)
    return pl.pallas_call(
        grad_a_kernel,
        grid_spec=pltpu.PrefetchScalarGridSpec(
            num_scalar_prefetch=1,
            grid=(count,),
            in_specs=[
                pl.BlockSpec((tokens, width), lambda i, p: (0, p[0] ^ (first + step * i))),
                pl.BlockSpec((tokens, rank), lambda i, p: (0, 0)),
            ],
            out_specs=[spec, spec],
            scratch_shapes=[pltpu.VMEM((width, rank), jnp.float32)],
        ),
        out_shape=[shape, shape],
        cost_estimate=pl.CostEstimate(
            flops=2 * tokens * width * rank * count,
            bytes_accessed=2 * (tokens + rank) * width * count,
            transcendentals=0,
        ),
        name="grad_a",
    )(pos, activations, err)


def grad_b_kernel(pos, low, other, coefficient, grad, loss, keep, send, whole):
    weighted = (coefficient[...] * (low[...] + other[...])).astype(jnp.bfloat16)
    whole[...] = lax.dot_general(
        weighted, grad[...], (((0,), (0,)), ((), ())), preferred_element_type=jnp.float32
    )
    depth, rows = keep.shape[:2]
    width = grad.shape[1]
    lane = lax.broadcasted_iota(jnp.int32, (rows, lanes), 1)
    value = jnp.broadcast_to(loss[...], (rows, lanes))
    parts = thirds(value, lane)
    for dk, out in enumerate((keep, send)):
        for r in range(depth):
            at = ((pos[0] ^ r) * 2 + (pos[2] ^ dk)) * rows
            out[r, :, :width] = whole[pl.ds(pl.multiple_of(at, rows), rows), :].astype(out.dtype)
            out[r, :, width:] = parts.astype(out.dtype)


def thirds(value, lane):
    high = value.astype(jnp.bfloat16).astype(jnp.float32)
    middle = (value - high).astype(jnp.bfloat16).astype(jnp.float32)
    low = value - high - middle
    zero = jnp.zeros_like(value)
    return jnp.where(
        lane == 0, high, jnp.where(lane == 1, middle, jnp.where(lane == 2, low, zero))
    )


def grad_b_part(pos, low, other, coefficient, grad, loss, depth):
    tokens, rank = low.shape
    width = grad.shape[1]
    rows = rank // (2 * depth)
    shape = (depth, rows, width + lanes)
    return pl.pallas_call(
        grad_b_kernel,
        in_specs=[pl.BlockSpec(memory_space=pltpu.SMEM)]
        + [pl.BlockSpec(memory_space=pltpu.VMEM)] * 5,
        out_shape=[
            jax.ShapeDtypeStruct(shape, jnp.float32),
            jax.ShapeDtypeStruct(shape, jnp.bfloat16),
        ],
        scratch_shapes=[pltpu.VMEM((rank, width), jnp.float32)],
        cost_estimate=pl.CostEstimate(
            flops=2 * tokens * width * rank,
            bytes_accessed=2 * tokens * width + 6 * rank * width,
            transcendentals=0,
        ),
        name="grad_b",
    )(pos, low, other, coefficient, grad, loss)


def chip_sum_kernel(keep, got, *outs):
    width = keep.shape[2] - lanes
    lane = lax.broadcasted_iota(jnp.int32, (keep.shape[1], lanes), 1)
    for r, out in enumerate(outs):
        total = keep[r] + got[r].astype(jnp.float32)
        out[:, :width] = total[:, :width].astype(out.dtype)
        value = jnp.sum(total[:, width:], axis=1, keepdims=True)
        out[:, width:] = thirds(jnp.broadcast_to(value, lane.shape), lane).astype(out.dtype)


def chip_sum(keep, got):
    depth, rows, width = keep.shape
    return pl.pallas_call(
        chip_sum_kernel,
        out_shape=[jax.ShapeDtypeStruct((rows, width), jnp.bfloat16)] * depth,
        name="chip_sum",
    )(keep, got)


def fill_kernel(pos, own, other, out):
    depth, rows = own.shape[:2]
    for dk, source in enumerate((own, other)):
        for r in range(depth):
            at = ((pos[0] ^ r) * 2 + (pos[2] ^ dk)) * rows
            out[pl.ds(pl.multiple_of(at, rows), rows), :] = source[r].astype(jnp.float32)


def fill(pos, own, other):
    depth, rows, width = own.shape
    return pl.pallas_call(
        fill_kernel,
        in_specs=[pl.BlockSpec(memory_space=pltpu.SMEM)]
        + [pl.BlockSpec(memory_space=pltpu.VMEM)] * 2,
        out_shape=jax.ShapeDtypeStruct((2 * depth * rows, width), jnp.float32),
        name="fill",
    )(pos, own, other)


def placed(activations, output_gradient, adapter_a, adapter_b, log_ratio, lengths, rewards):
    size = lax.axis_size("dp")
    depth = size // (2 * cores)
    rows, rank = adapter_a.shape[1:]
    tokens = activations.shape[0]
    position = lax.axis_index("dp")
    k = position % cores
    y = position // cores % 2
    z = position // (2 * cores)
    pos = jnp.stack([z, y, k]).astype(jnp.int32)
    everyone = [(zz, yy, kk) for zz in range(depth) for yy in range(2) for kk in range(cores)]
    number = lambda zz, yy, kk: (zz * 2 + yy) * cores + kk

    def move(value, target):
        return lax.ppermute(value, "dp", [(number(*at), number(*target(*at))) for at in everyone])

    to_core = lambda value: move(value, lambda zz, yy, kk: (zz, yy, kk ^ 1))
    to_y = lambda value: move(value, lambda zz, yy, kk: (zz, yy ^ 1, kk))
    to_z = lambda value, r: move(value, lambda zz, yy, kk: (zz ^ r, yy, kk))
    across = lambda value, r: move(value, lambda zz, yy, kk: (zz ^ r, kk, yy))
    other_tensor = lambda value: lax.ppermute(value, "tensor", [(0, 1), (1, 0)])

    gathered = [adapter_a[0]]
    for r in range(1, depth):
        gathered.append(to_z(gathered[0], r))
    by_y = [to_y(value) for value in gathered]
    slices = []
    for own, over in zip(gathered, by_y):
        slices.append([own, to_core(own), over, to_core(over)])

    coefficient, loss, factor = own_terms(log_ratio, lengths, rewards)
    back = lax.dot_general(
        output_gradient, adapter_b, (((1,), (1,)), ((), ())), preferred_element_type=jnp.float32
    )
    back = back + other_tensor(back)
    err = (adapter_scale_factor * coefficient[:, None] * back).astype(jnp.bfloat16)

    half = depth // 2
    groups = [list(range(depth - 1, half - 1, -1)), list(range(half - 1, -1, -1))]
    f32 = lambda value: value.astype(jnp.float32)
    sums = {}
    for group in groups:
        keep, send = grad_a_part(pos, activations, err, group, rows)
        total = f32(keep) + f32(to_core(send))
        got = to_y(total[1].astype(jnp.bfloat16))
        for index, r in enumerate(group):
            sums[r] = total[0][index] + f32(got[index])
    grad_a = sums[0]
    for r in range(1, depth):
        grad_a = grad_a + f32(to_z(sums[r].astype(jnp.bfloat16), r))

    low = low_rank_part(pos, activations, list(range(half)), sum(slices[:half], []))
    low = low_rank_part(pos, activations, list(range(half, depth)), sum(slices[half:], []), low)
    scale = (adapter_scale_factor * factor * coefficient)[:, None]
    keep, send = grad_b_part(
        pos, low, other_tensor(low), scale, output_gradient, loss.reshape(1, 1), depth
    )
    pieces = chip_sum(keep, to_core(send))
    total = 0.0
    for r in range(depth):
        total = total + f32(across(pieces[r], r))
    total = total + to_core(total)
    loss = jnp.sum(total[0, -lanes:])
    chunk = total[:, :-lanes].astype(jnp.bfloat16)
    own = jnp.stack([across(chunk, r) for r in range(depth)])
    grad_b = fill(pos, own, to_core(own))
    return ((factor * grad_a)[None], grad_b, factor * loss)


def local(*args):
    activations, _, adapter_a = args[:3]
    size = lax.axis_size("dp")
    depth = size // (2 * cores)
    rows, rank = adapter_a.shape[1:]
    fits = (
        lax.axis_size("tensor") == 2
        and size == 2 * cores * depth
        and depth > 1
        and depth & (depth - 1) == 0
        and depth <= 8
        and rows % 16 == 0
        and 4 * rows % lanes == 0
        and rank == lanes
        and rank % (32 * depth) == 0
    )
    return placed(*args) if fits else general(*args)


def solution(mesh):
    in_specs = (
        P("dp", "tensor"),
        P("dp", "tensor"),
        P("tensor", "dp", None),
        P(None, "tensor"),
        P("dp"),
        P(),
        P(),
    )
    out_specs = (P("tensor", "dp", None), P(None, "tensor"), P())
    return jax.shard_map(local, mesh=mesh, in_specs=in_specs, out_specs=out_specs, check_vma=False)
```

```python
import functools

import jax
import jax.numpy as jnp
from jax import lax
from jax.experimental import pallas as pl
from jax.experimental.pallas import tpu as pltpu
from jax.sharding import PartitionSpec as P


clip_eps = 0.2
adapter_scale_factor = 2.0
cores = 2
lanes = 128


def slot_terms(length_row, reward_row, log_ratio, offset):
    reward = reward_row.astype(jnp.float32)
    center = jnp.mean(reward)
    spread = jnp.mean((reward - center) * (reward - center))
    advantage = (reward - center) / jnp.sqrt(spread + 1.0)
    ends = jnp.cumsum(length_row)
    starts = ends - length_row
    slots = jnp.arange(log_ratio.shape[0], dtype=jnp.int32) + offset
    member = ((slots[None, :] >= starts[:, None]) & (slots[None, :] < ends[:, None])).astype(
        jnp.float32
    )
    live = jnp.sum(member, axis=0)
    token_adv = jnp.sum(member * advantage[:, None], axis=0)
    ratio = jnp.exp(log_ratio)
    unclipped = ratio * token_adv
    clipped = jnp.clip(ratio, 1.0 - clip_eps, 1.0 + clip_eps) * token_adv
    token_loss = -jnp.minimum(unclipped, clipped)
    slope = jnp.where(unclipped <= clipped, -unclipped, jnp.zeros_like(unclipped))
    return (live * slope, jnp.sum(live * token_loss))


def own_terms(log_ratio, lengths, rewards):
    tokens = log_ratio.shape[0]
    groups = lengths.shape[0]
    per_group = lax.axis_size("dp") // groups
    position = lax.axis_index("dp")
    group_id = position // per_group
    offset = position % per_group * tokens
    length_row = lax.dynamic_index_in_dim(lengths, group_id, 0, keepdims=False)
    reward_row = lax.dynamic_index_in_dim(rewards, group_id, 0, keepdims=False)
    coefficient, loss = slot_terms(length_row, reward_row, log_ratio, offset)
    live = jnp.sum(jnp.minimum(jnp.sum(lengths, axis=1), per_group * tokens))
    return coefficient, loss, groups / live.astype(jnp.float32)


def general(activations, output_gradient, adapter_a, adapter_b, log_ratio, lengths, rewards):
    coefficient, loss, factor = own_terms(log_ratio, lengths, rewards)
    partial_low = jnp.dot(
        activations,
        lax.all_gather(adapter_a, "dp", axis=1, tiled=True)[0],
        preferred_element_type=jnp.float32,
    )
    partial_back = lax.dot_general(
        output_gradient, adapter_b, (((1,), (1,)), ((), ())), preferred_element_type=jnp.float32
    )
    low_rank, back = lax.psum((partial_low, partial_back), "tensor")
    error_rows = (adapter_scale_factor * coefficient[:, None] * back).astype(jnp.bfloat16)
    grad_b = adapter_scale_factor * jnp.einsum(
        "tr,td->rd",
        coefficient[:, None] * low_rank,
        output_gradient.astype(jnp.float32),
        precision=lax.Precision.HIGHEST,
    )
    grad_a = lax.psum_scatter(
        lax.dot_general(
            activations, error_rows, (((0,), (0,)), ((), ())), preferred_element_type=jnp.float32
        ),
        "dp",
        scatter_dimension=0,
        tiled=True,
    )
    grad_b, loss = lax.psum((grad_b, loss), "dp")
    return ((factor * grad_a)[None], factor * grad_b, factor * loss)


vmem = pl.BlockSpec(memory_space=pltpu.VMEM)


def limit(size):
    return size + 4 * 2**20


def place():
    position = lax.axis_index("dp")
    return position // (2 * cores), position // cores % 2, position % cores


def segment(dy, dk, rows):
    _, y, k = place()
    return pl.ds(pl.multiple_of((lax.bitwise_xor(y, dy) * 2 + lax.bitwise_xor(k, dk)) * rows, 16), rows)


def terms_kernel(lengths, rewards, log_ratio, _, spread_out, stats, *, per_group):
    groups, count = lengths.shape
    lines = log_ratio.shape[0]
    shape = (lines, lanes)
    tokens = lines * lanes
    position = lax.axis_index("dp")
    group = position // per_group
    value = [jnp.full(shape, rewards[group, i], jnp.int32).astype(jnp.float32) for i in range(count)]
    center = sum(value) / count
    spread = sum((v - center) * (v - center) for v in value) / count
    root = jnp.sqrt(spread + 1.0)
    slots = (
        lax.broadcasted_iota(jnp.int32, shape, 0) * lanes
        + lax.broadcasted_iota(jnp.int32, shape, 1)
        + position % per_group * tokens
    )
    token_adv = jnp.zeros(shape, jnp.float32)
    live = jnp.zeros(shape, jnp.float32)
    start = 0
    for i in range(count):
        end = start + lengths[group, i]
        member = ((slots >= start) & (slots < end)).astype(jnp.float32)
        token_adv = token_adv + member * ((value[i] - center) / root)
        live = live + member
        start = end
    ratio = jnp.exp(log_ratio[...])
    unclipped = ratio * token_adv
    clipped = jnp.clip(ratio, 1.0 - clip_eps, 1.0 + clip_eps) * token_adv
    loss = jnp.sum(live * -jnp.minimum(unclipped, clipped))
    coefficient = live * jnp.where(unclipped <= clipped, -unclipped, jnp.zeros(shape, jnp.float32))
    for line in range(lines):
        row = jnp.broadcast_to(coefficient[line : line + 1, :], (lanes, lanes))
        spread_out[line * lanes : (line + 1) * lanes, :] = row.T
    total = 0
    for g in range(groups):
        size = 0
        for i in range(count):
            size = size + lengths[g, i]
        total = total + jnp.minimum(size, per_group * tokens)
    stats[0] = jnp.broadcast_to(loss, stats.shape[1:])
    stats[1] = groups / jnp.full(stats.shape[1:], total, jnp.int32).astype(jnp.float32)


def terms(log_ratio, lengths, rewards, activations):
    tokens = log_ratio.shape[0]
    per_group = lax.axis_size("dp") // lengths.shape[0]
    return pl.pallas_call(
        functools.partial(terms_kernel, per_group=per_group),
        in_specs=[pl.BlockSpec(memory_space=pltpu.SMEM)] * 2
        + [vmem] * 2,
        out_specs=[vmem] * 2,
        out_shape=[
            jax.ShapeDtypeStruct((tokens, lanes), jnp.float32),
            jax.ShapeDtypeStruct((2, 8, lanes), jnp.float32),
        ],
        name="terms",
        compiler_params=pltpu.CompilerParams(vmem_limit_bytes=limit(2 * activations.size)),
    )(lengths, rewards, log_ratio.reshape(tokens // lanes, lanes), activations)


def back_kernel(grad, factor, out):
    out[...] = lax.dot_general(
        grad[...], factor[...], (((1,), (1,)), ((), ())), preferred_element_type=jnp.float32
    )


def back_part(grad, factor):
    tokens, width = grad.shape
    rank = factor.shape[0]
    return pl.pallas_call(
        back_kernel,
        in_specs=[vmem] * 2,
        out_specs=vmem,
        out_shape=jax.ShapeDtypeStruct((tokens, rank), jnp.float32),
        cost_estimate=pl.CostEstimate(
            flops=2 * tokens * width * rank,
            bytes_accessed=2 * (tokens + rank) * width,
            transcendentals=0,
        ),
        name="back",
        compiler_params=pltpu.CompilerParams(
            vmem_limit_bytes=limit(2 * (tokens + rank) * width)
        ),
    )(grad, factor)


def tile_of(width):
    blocks = width // lanes
    return next(blocks // n for n in range(3, blocks + 1) if blocks % n == 0) * lanes


def columns(r, t, width, tile):
    at = lax.bitwise_xor(place()[0], r) * width + t * tile
    return pl.ds(pl.multiple_of(at, lanes), tile)


def low_rank_kernel(rounds, chained, acts, *refs):
    count = len(rounds)
    slices = refs[: 4 * count]
    out, whole = refs[-2:]
    rows = slices[0].shape[0]
    width = 4 * rows
    tile = tile_of(width)
    total = refs[4 * count][...] if chained else None
    for index, r in enumerate(rounds):
        for dy in range(2):
            for dk in range(2):
                whole[index, segment(dy, dk, rows)] = slices[4 * index + 2 * dy + dk][...]
        for t in range(width // tile):
            part = jnp.dot(
                acts[:, columns(r, t, width, tile)],
                whole[index, t * tile : (t + 1) * tile, :],
                preferred_element_type=jnp.float32,
            )
            total = part if total is None else total + part
    out[...] = total


def low_rank_part(activations, rounds, slices, before=None):
    tokens = activations.shape[0]
    rows, rank = slices[0].shape
    width = 4 * rows
    count = len(rounds)
    extra = () if before is None else (before,)
    return pl.pallas_call(
        functools.partial(low_rank_kernel, rounds, before is not None),
        in_specs=[vmem] * (1 + len(slices) + len(extra)),
        out_specs=vmem,
        scratch_shapes=[pltpu.VMEM((count, width, rank), jnp.bfloat16)],
        out_shape=jax.ShapeDtypeStruct((tokens, rank), jnp.float32),
        cost_estimate=pl.CostEstimate(
            flops=2 * tokens * width * rank * count,
            bytes_accessed=2 * (tokens + rank) * width * count,
            transcendentals=0,
        ),
        name="low_rank",
        compiler_params=pltpu.CompilerParams(
            vmem_limit_bytes=limit(2 * activations.size + 4 * count * width * rank)
        ),
    )(activations, *slices, *extra)


def grad_a_kernel(rounds, acts, coefficient, back, other, keep, send, whole):
    rows = keep.shape[2]
    width = 4 * rows
    tile = tile_of(width)
    scaled = adapter_scale_factor * coefficient[...] * (back[...] + other[...])
    err = scaled.astype(jnp.bfloat16)
    for index, r in enumerate(rounds):
        for t in range(width // tile):
            part = lax.dot_general(
                acts[:, columns(r, t, width, tile)],
                err,
                (((0,), (0,)), ((), ())),
                preferred_element_type=jnp.float32,
            )
            whole[index, t * tile : (t + 1) * tile, :] = part.astype(jnp.bfloat16)
        for dk, out in enumerate((keep, send)):
            for dy in range(2):
                out[index, dy] = whole[index, segment(dy, dk, rows)]


def grad_a_part(activations, coefficient, back, other, rounds, rows):
    tokens, rank = back.shape
    width = 4 * rows
    count = len(rounds)
    shape = jax.ShapeDtypeStruct((count, 2, rows, rank), jnp.bfloat16)
    return pl.pallas_call(
        functools.partial(grad_a_kernel, rounds),
        in_specs=[vmem] * 4,
        out_specs=[vmem] * 2,
        scratch_shapes=[pltpu.VMEM((count, width, rank), jnp.bfloat16)],
        out_shape=[shape, shape],
        cost_estimate=pl.CostEstimate(
            flops=2 * tokens * width * rank * count,
            bytes_accessed=2 * (tokens + rank) * width * count,
            transcendentals=0,
        ),
        name="grad_a",
        compiler_params=pltpu.CompilerParams(
            vmem_limit_bytes=limit(2 * activations.size + 4 * count * width * rank)
        ),
    )(activations, coefficient, back, other)


def grad_b_kernel(low, other, coefficient, stats, grad, keep, send, whole):
    depth, rows = keep.shape[:2]
    width = grad.shape[1]
    tile = tile_of(width)
    scale = adapter_scale_factor * stats[1][:1] * coefficient[...]
    weighted = (scale * (low[...] + other[...])).astype(jnp.bfloat16)
    shape = (rows, lanes)
    parts = thirds(
        jnp.broadcast_to(stats[0][:1], shape), lax.broadcasted_iota(jnp.int32, shape, 1)
    )
    for t in range(width // tile):
        whole[:, t * tile : (t + 1) * tile] = lax.dot_general(
            weighted,
            grad[:, t * tile : (t + 1) * tile],
            (((0,), (0,)), ((), ())),
            preferred_element_type=jnp.float32,
        )
    z, _, k = place()
    for dk, out in enumerate((keep, send)):
        for r in range(depth):
            at = (lax.bitwise_xor(z, r) * 2 + lax.bitwise_xor(k, dk)) * rows
            out[r, :, :width] = whole[pl.ds(pl.multiple_of(at, rows), rows), :].astype(out.dtype)
            out[r, :, width:] = parts.astype(out.dtype)


def grad_b_part(low, other, coefficient, stats, grad, depth):
    tokens, rank = low.shape
    width = grad.shape[1]
    rows = rank // (2 * depth)
    shape = (depth, rows, width + lanes)
    return pl.pallas_call(
        grad_b_kernel,
        in_specs=[vmem] * 5,
        out_specs=[vmem] * 2,
        out_shape=[
            jax.ShapeDtypeStruct(shape, jnp.float32),
            jax.ShapeDtypeStruct(shape, jnp.bfloat16),
        ],
        scratch_shapes=[pltpu.VMEM((rank, width), jnp.float32)],
        cost_estimate=pl.CostEstimate(
            flops=2 * tokens * width * rank,
            bytes_accessed=2 * tokens * width + 6 * rank * width,
            transcendentals=0,
        ),
        name="grad_b",
        compiler_params=pltpu.CompilerParams(vmem_limit_bytes=limit(10 * rank * width)),
    )(low, other, coefficient, stats, grad)


def thirds(value, lane):
    high = value.astype(jnp.bfloat16).astype(jnp.float32)
    middle = (value - high).astype(jnp.bfloat16).astype(jnp.float32)
    low = value - high - middle
    zero = jnp.zeros_like(value)
    return jnp.where(
        lane == 0, high, jnp.where(lane == 1, middle, jnp.where(lane == 2, low, zero))
    )


def chip_sum_kernel(keep, got, *outs):
    width = keep.shape[2] - lanes
    lane = lax.broadcasted_iota(jnp.int32, (keep.shape[1], lanes), 1)
    for r, out in enumerate(outs):
        total = keep[r] + got[r].astype(jnp.float32)
        out[:, :width] = total[:, :width].astype(out.dtype)
        value = jnp.sum(total[:, width:], axis=1, keepdims=True)
        out[:, width:] = thirds(jnp.broadcast_to(value, lane.shape), lane).astype(out.dtype)


def chip_sum(keep, got):
    depth, rows, width = keep.shape
    return pl.pallas_call(
        chip_sum_kernel,
        out_shape=[jax.ShapeDtypeStruct((rows, width), jnp.bfloat16)] * depth,
        name="chip_sum",
        compiler_params=pltpu.CompilerParams(vmem_limit_bytes=limit(6 * 2**20)),
    )(keep, got)


def fill_kernel(own, other, out):
    depth, rows = own.shape[:2]
    z, _, k = place()
    for dk, source in enumerate((own, other)):
        for r in range(depth):
            at = (lax.bitwise_xor(z, r) * 2 + lax.bitwise_xor(k, dk)) * rows
            out[pl.ds(pl.multiple_of(at, rows), rows), :] = source[r].astype(jnp.float32)


def fill(own, other):
    depth, rows, width = own.shape
    return pl.pallas_call(
        fill_kernel,
        out_shape=jax.ShapeDtypeStruct((2 * depth * rows, width), jnp.float32),
        name="fill",
        compiler_params=pltpu.CompilerParams(vmem_limit_bytes=limit(6 * 2**20)),
    )(own, other)


def placed(activations, output_gradient, adapter_a, adapter_b, log_ratio, lengths, rewards):
    size = lax.axis_size("dp")
    depth = size // (2 * cores)
    rows, _ = adapter_a.shape[1:]
    everyone = [(zz, yy, kk) for zz in range(depth) for yy in range(2) for kk in range(cores)]
    number = lambda zz, yy, kk: (zz * 2 + yy) * cores + kk
    f32 = lambda value: value.astype(jnp.float32)
    half_width = lambda value: value.astype(jnp.bfloat16)

    def move(value, target):
        pairs = [(number(*at), number(*target(*at))) for at in everyone]
        return lax.ppermute(value, "dp", pairs)

    to_core = lambda value: move(value, lambda zz, yy, kk: (zz, yy, kk ^ 1))
    to_y = lambda value: move(value, lambda zz, yy, kk: (zz, yy ^ 1, kk))
    to_z = lambda value, r: move(value, lambda zz, yy, kk: (zz ^ r, yy, kk))
    across = lambda value, r: move(value, lambda zz, yy, kk: (zz ^ r, kk, yy))

    def other_tensor(value):
        return lax.ppermute(value, "tensor", [(0, 1), (1, 0)])

    bit = depth // 2
    have = {0: adapter_a[0]}
    while bit:
        for r in sorted(have):
            have[r ^ bit] = to_z(have[r], bit)
        bit //= 2
    slices = []
    for r in range(depth):
        over = to_y(have[r])
        slices.append([have[r], to_core(have[r]), over, to_core(over)])

    back = back_part(output_gradient, adapter_b)
    coefficient, stats = terms(log_ratio, lengths, rewards, activations)
    other_back = other_tensor(back)

    order = [r for r in range(depth - 1, -1, -1)]
    sums = {}
    for start in range(0, depth, 2):
        group = order[start : start + 2]
        keep, send = grad_a_part(
            activations, coefficient, back, other_back, group, rows
        )
        got = to_core(send)
        for index, r in enumerate(group):
            sums[r] = f32(keep[index]) + f32(got[index])
    got = to_y(half_width(jnp.stack([sums[1][1], sums[0][1]])))
    near = half_width(sums.pop(1)[0] + f32(got[0]))
    own = sums.pop(0)[0] + f32(got[1])
    bit = 1
    while 2 * bit < depth:
        for r in order:
            if r & bit and r in sums:
                got = to_z(half_width(sums.pop(r)), bit)
                sums[r ^ bit] = sums[r ^ bit] + f32(got)
        bit *= 2
    for r in list(sums):
        got = to_y(half_width(sums[r][1]))
        sums[r] = sums[r][0] + f32(got)
    near = to_z(near, 1)
    last = to_z(half_width(sums[bit]), bit)
    factor = stats[1, 0, 0]
    grad_a = factor * ((own + f32(near)) + f32(last))

    cut = depth - 1
    low = low_rank_part(activations, list(range(cut)), sum(slices[:cut], []))
    low = low_rank_part(activations, list(range(cut, depth)), sum(slices[cut:], []), low)
    other = other_tensor(low)
    keep, send = grad_b_part(low, other, coefficient, stats, output_gradient, depth)
    got = to_core(send)
    pieces = chip_sum(keep, got)
    total = 0.0
    for r in range(depth):
        total = total + f32(across(pieces[r], r))
    total = total + to_core(total)
    loss = jnp.sum(total[0, -lanes:])
    chunk = half_width(total[:, :-lanes])
    own = jnp.stack([across(chunk, r) for r in range(depth)])
    grad_b = fill(own, to_core(own))
    return (grad_a[None], grad_b, factor * loss)


def local(*args):
    _, _, adapter_a = args[:3]
    size = lax.axis_size("dp")
    depth = size // (2 * cores)
    rows, rank = adapter_a.shape[1:]
    fits = (
        lax.axis_size("tensor") == 2
        and size == 2 * cores * depth
        and depth == 4
        and rows % 16 == 0
        and 4 * rows % lanes == 0
        and rank == lanes
        and rank % (32 * depth) == 0
        and args[4].shape[0] % lanes == 0
    )
    return placed(*args) if fits else general(*args)


def solution(mesh):
    in_specs = (
        P("dp", "tensor"),
        P("dp", "tensor"),
        P("tensor", "dp", None),
        P(None, "tensor"),
        P("dp"),
        P(),
        P(),
    )
    out_specs = (P("tensor", "dp", None), P(None, "tensor"), P())

    return jax.shard_map(local, mesh=mesh, in_specs=in_specs, out_specs=out_specs, check_vma=False)
```

```python
import functools

import jax
import jax.numpy as jnp
from jax import lax
from jax.experimental import pallas as pl
from jax.experimental.pallas import tpu as pltpu
from jax.sharding import PartitionSpec as P


clip_eps = 0.2
adapter_scale_factor = 2.0
cores = 2
lanes = 128


def slot_terms(length_row, reward_row, log_ratio, offset):
    reward = reward_row.astype(jnp.float32)
    center = jnp.mean(reward)
    spread = jnp.mean((reward - center) * (reward - center))
    advantage = (reward - center) / jnp.sqrt(spread + 1.0)
    ends = jnp.cumsum(length_row)
    starts = ends - length_row
    slots = jnp.arange(log_ratio.shape[0], dtype=jnp.int32) + offset
    member = ((slots[None, :] >= starts[:, None]) & (slots[None, :] < ends[:, None])).astype(
        jnp.float32
    )
    live = jnp.sum(member, axis=0)
    token_adv = jnp.sum(member * advantage[:, None], axis=0)
    ratio = jnp.exp(log_ratio)
    unclipped = ratio * token_adv
    clipped = jnp.clip(ratio, 1.0 - clip_eps, 1.0 + clip_eps) * token_adv
    token_loss = -jnp.minimum(unclipped, clipped)
    slope = jnp.where(unclipped <= clipped, -unclipped, jnp.zeros_like(unclipped))
    return (live * slope, jnp.sum(live * token_loss))


def own_terms(log_ratio, lengths, rewards):
    tokens = log_ratio.shape[0]
    groups = lengths.shape[0]
    per_group = lax.axis_size("dp") // groups
    position = lax.axis_index("dp")
    group_id = position // per_group
    offset = position % per_group * tokens
    length_row = lax.dynamic_index_in_dim(lengths, group_id, 0, keepdims=False)
    reward_row = lax.dynamic_index_in_dim(rewards, group_id, 0, keepdims=False)
    coefficient, loss = slot_terms(length_row, reward_row, log_ratio, offset)
    live = jnp.sum(jnp.minimum(jnp.sum(lengths, axis=1), per_group * tokens))
    return coefficient, loss, groups / live.astype(jnp.float32)


def general(activations, output_gradient, adapter_a, adapter_b, log_ratio, lengths, rewards):
    coefficient, loss, factor = own_terms(log_ratio, lengths, rewards)
    partial_low = jnp.dot(
        activations,
        lax.all_gather(adapter_a, "dp", axis=1, tiled=True)[0],
        preferred_element_type=jnp.float32,
    )
    partial_back = lax.dot_general(
        output_gradient, adapter_b, (((1,), (1,)), ((), ())), preferred_element_type=jnp.float32
    )
    low_rank, back = lax.psum((partial_low, partial_back), "tensor")
    error_rows = (adapter_scale_factor * coefficient[:, None] * back).astype(jnp.bfloat16)
    grad_b = adapter_scale_factor * jnp.einsum(
        "tr,td->rd",
        coefficient[:, None] * low_rank,
        output_gradient.astype(jnp.float32),
        precision=lax.Precision.HIGHEST,
    )
    grad_a = lax.psum_scatter(
        lax.dot_general(
            activations, error_rows, (((0,), (0,)), ((), ())), preferred_element_type=jnp.float32
        ),
        "dp",
        scatter_dimension=0,
        tiled=True,
    )
    grad_b, loss = lax.psum((grad_b, loss), "dp")
    return ((factor * grad_a)[None], factor * grad_b, factor * loss)


vmem = pl.BlockSpec(memory_space=pltpu.VMEM)


def limit(size):
    return size + 4 * 2**20


def place():
    position = lax.axis_index("dp")
    return position // (2 * cores), position // cores % 2, position % cores


def segment(dy, dk, rows):
    _, y, k = place()
    return pl.ds(pl.multiple_of((lax.bitwise_xor(y, dy) * 2 + lax.bitwise_xor(k, dk)) * rows, 16), rows)


def terms_kernel(lengths, rewards, log_ratio, spread_out, stats, *, per_group):
    groups, count = lengths.shape
    lines = log_ratio.shape[0]
    shape = (lines, lanes)
    tokens = lines * lanes
    position = lax.axis_index("dp")
    group = position // per_group
    value = [jnp.full(shape, rewards[group, i], jnp.int32).astype(jnp.float32) for i in range(count)]
    center = sum(value) / count
    spread = sum((v - center) * (v - center) for v in value) / count
    root = jnp.sqrt(spread + 1.0)
    slots = (
        lax.broadcasted_iota(jnp.int32, shape, 0) * lanes
        + lax.broadcasted_iota(jnp.int32, shape, 1)
        + position % per_group * tokens
    )
    token_adv = jnp.zeros(shape, jnp.float32)
    live = jnp.zeros(shape, jnp.float32)
    start = 0
    for i in range(count):
        end = start + lengths[group, i]
        member = ((slots >= start) & (slots < end)).astype(jnp.float32)
        token_adv = token_adv + member * ((value[i] - center) / root)
        live = live + member
        start = end
    ratio = jnp.exp(log_ratio[...])
    unclipped = ratio * token_adv
    clipped = jnp.clip(ratio, 1.0 - clip_eps, 1.0 + clip_eps) * token_adv
    loss = jnp.sum(live * -jnp.minimum(unclipped, clipped))
    coefficient = live * jnp.where(unclipped <= clipped, -unclipped, jnp.zeros(shape, jnp.float32))
    for line in range(lines):
        row = jnp.broadcast_to(coefficient[line : line + 1, :], (lanes, lanes))
        spread_out[line * lanes : (line + 1) * lanes, :] = row.T
    total = 0
    for g in range(groups):
        size = 0
        for i in range(count):
            size = size + lengths[g, i]
        total = total + jnp.minimum(size, per_group * tokens)
    stats[0] = jnp.broadcast_to(loss, stats.shape[1:])
    stats[1] = groups / jnp.full(stats.shape[1:], total, jnp.int32).astype(jnp.float32)


def terms(log_ratio, lengths, rewards):
    tokens = log_ratio.shape[0]
    per_group = lax.axis_size("dp") // lengths.shape[0]
    return pl.pallas_call(
        functools.partial(terms_kernel, per_group=per_group),
        in_specs=[pl.BlockSpec(memory_space=pltpu.SMEM)] * 2
        + [vmem],
        out_specs=[vmem] * 2,
        out_shape=[
            jax.ShapeDtypeStruct((tokens, lanes), jnp.float32),
            jax.ShapeDtypeStruct((2, 8, lanes), jnp.float32),
        ],
        name="terms",
        compiler_params=pltpu.CompilerParams(vmem_limit_bytes=limit(2**20)),
    )(lengths, rewards, log_ratio.reshape(tokens // lanes, lanes))


def lead_kernel(out):
    out[...] = jnp.zeros(out.shape, out.dtype)


def lead():
    return pl.pallas_call(
        lead_kernel,
        out_specs=vmem,
        out_shape=jax.ShapeDtypeStruct((8, lanes), jnp.float32),
        cost_estimate=pl.CostEstimate(flops=10**10, bytes_accessed=0, transcendentals=0),
        name="lead",
        compiler_params=pltpu.CompilerParams(vmem_limit_bytes=limit(0)),
    )()


def back_kernel(grad, factor, _, out):
    out[...] = lax.dot_general(
        grad[...], factor[...], (((1,), (1,)), ((), ())), preferred_element_type=jnp.float32
    )


def back_part(grad, factor, first):
    tokens, width = grad.shape
    rank = factor.shape[0]
    return pl.pallas_call(
        back_kernel,
        in_specs=[vmem] * 3,
        out_specs=vmem,
        out_shape=jax.ShapeDtypeStruct((tokens, rank), jnp.float32),
        cost_estimate=pl.CostEstimate(
            flops=2 * tokens * width * rank,
            bytes_accessed=2 * (tokens + rank) * width,
            transcendentals=0,
        ),
        name="back",
        compiler_params=pltpu.CompilerParams(
            vmem_limit_bytes=limit(2 * (tokens + rank) * width)
        ),
    )(grad, factor, first)


def tile_of(width):
    blocks = width // lanes
    return next(blocks // n for n in range(3, blocks + 1) if blocks % n == 0) * lanes


def columns(r, t, width, tile):
    at = lax.bitwise_xor(place()[0], r) * width + t * tile
    return pl.ds(pl.multiple_of(at, lanes), tile)


def low_rank_kernel(rounds, chained, acts, *refs):
    count = len(rounds)
    slices = refs[: 4 * count]
    out, sent, whole = refs[-3:]
    rows = slices[0].shape[0]
    width = 4 * rows
    tile = tile_of(width)
    total = refs[4 * count][...] if chained else None
    for index, r in enumerate(rounds):
        for dy in range(2):
            for dk in range(2):
                whole[index, segment(dy, dk, rows)] = slices[4 * index + 2 * dy + dk][...]
        for t in range(width // tile):
            part = jnp.dot(
                acts[:, columns(r, t, width, tile)],
                whole[index, t * tile : (t + 1) * tile, :],
                preferred_element_type=jnp.float32,
            )
            total = part if total is None else total + part
    out[...] = total
    sent[...] = total.astype(sent.dtype)


def low_rank_part(activations, rounds, slices, before=None):
    tokens = activations.shape[0]
    rows, rank = slices[0].shape
    width = 4 * rows
    count = len(rounds)
    extra = () if before is None else (before,)
    return pl.pallas_call(
        functools.partial(low_rank_kernel, rounds, before is not None),
        in_specs=[vmem] * (1 + len(slices) + len(extra)),
        out_specs=[vmem] * 2,
        scratch_shapes=[pltpu.VMEM((count, width, rank), jnp.bfloat16)],
        out_shape=[
            jax.ShapeDtypeStruct((tokens, rank), jnp.float32),
            jax.ShapeDtypeStruct((tokens, rank), jnp.bfloat16),
        ],
        cost_estimate=pl.CostEstimate(
            flops=2 * tokens * width * rank * count,
            bytes_accessed=2 * (tokens + rank) * width * count,
            transcendentals=0,
        ),
        name="low_rank",
        compiler_params=pltpu.CompilerParams(
            vmem_limit_bytes=limit(2 * activations.size + 4 * count * width * rank)
        ),
    )(activations, *slices, *extra)


def grad_a_kernel(order, acts, coefficient, back, other, *refs):
    outs, whole = refs[:-1], refs[-1]
    rows = outs[0].shape[2]
    width = 4 * rows
    tile = tile_of(width)
    scaled = adapter_scale_factor * coefficient[...] * (back[...] + other[...])
    err = scaled.astype(jnp.bfloat16)
    for index, r in enumerate(order):
        for t in range(width // tile):
            part = lax.dot_general(
                acts[:, columns(r, t, width, tile)],
                err,
                (((0,), (0,)), ((), ())),
                preferred_element_type=jnp.float32,
            )
            whole[index % 2, t * tile : (t + 1) * tile, :] = part.astype(jnp.bfloat16)
        for dk in range(2):
            for dy in range(2):
                outs[index // 2 * 2 + dk][index % 2, dy] = whole[
                    index % 2, segment(dy, dk, rows)
                ]


def grad_a_part(activations, coefficient, back, other, order, rows):
    tokens, rank = back.shape
    width = 4 * rows
    count = len(order)
    shape = jax.ShapeDtypeStruct((2, 2, rows, rank), jnp.bfloat16)
    return pl.pallas_call(
        functools.partial(grad_a_kernel, order),
        in_specs=[vmem] * 4,
        out_specs=[vmem] * count,
        scratch_shapes=[pltpu.VMEM((2, width, rank), jnp.bfloat16)],
        out_shape=[shape] * count,
        cost_estimate=pl.CostEstimate(
            flops=2 * tokens * width * rank * count,
            bytes_accessed=2 * (tokens + rank) * width * count,
            transcendentals=0,
        ),
        name="grad_a",
        compiler_params=pltpu.CompilerParams(
            vmem_limit_bytes=limit(2 * activations.size + 4 * count * width * rank)
        ),
    )(activations, coefficient, back, other)


def grad_b_kernel(low, other, coefficient, stats, grad, keep, send, whole):
    depth, rows = keep.shape[:2]
    width = grad.shape[1]
    tile = tile_of(width)
    scale = adapter_scale_factor * stats[1][:1] * coefficient[...]
    weighted = (scale * (low[...] + other[...].astype(jnp.float32))).astype(jnp.bfloat16)
    shape = (rows, lanes)
    parts = thirds(
        jnp.broadcast_to(stats[0][:1], shape), lax.broadcasted_iota(jnp.int32, shape, 1)
    )
    for t in range(width // tile):
        whole[:, t * tile : (t + 1) * tile] = lax.dot_general(
            weighted,
            grad[:, t * tile : (t + 1) * tile],
            (((0,), (0,)), ((), ())),
            preferred_element_type=jnp.float32,
        )
    z, _, k = place()
    for dk, out in enumerate((keep, send)):
        for r in range(depth):
            at = (lax.bitwise_xor(z, r) * 2 + lax.bitwise_xor(k, dk)) * rows
            out[r, :, :width] = whole[pl.ds(pl.multiple_of(at, rows), rows), :].astype(out.dtype)
            out[r, :, width:] = parts.astype(out.dtype)


def grad_b_part(low, other, coefficient, stats, grad, depth):
    tokens, rank = low.shape
    width = grad.shape[1]
    rows = rank // (2 * depth)
    shape = (depth, rows, width + lanes)
    return pl.pallas_call(
        grad_b_kernel,
        in_specs=[vmem] * 5,
        out_specs=[vmem] * 2,
        out_shape=[
            jax.ShapeDtypeStruct(shape, jnp.float32),
            jax.ShapeDtypeStruct(shape, jnp.bfloat16),
        ],
        scratch_shapes=[pltpu.VMEM((rank, width), jnp.float32)],
        cost_estimate=pl.CostEstimate(
            flops=2 * tokens * width * rank,
            bytes_accessed=2 * tokens * width + 6 * rank * width,
            transcendentals=0,
        ),
        name="grad_b",
        compiler_params=pltpu.CompilerParams(vmem_limit_bytes=limit(10 * rank * width)),
    )(low, other, coefficient, stats, grad)


def thirds(value, lane):
    high = value.astype(jnp.bfloat16).astype(jnp.float32)
    middle = (value - high).astype(jnp.bfloat16).astype(jnp.float32)
    low = value - high - middle
    zero = jnp.zeros_like(value)
    return jnp.where(
        lane == 0, high, jnp.where(lane == 1, middle, jnp.where(lane == 2, low, zero))
    )


def chip_sum_kernel(keep, got, *outs):
    width = keep.shape[2] - lanes
    lane = lax.broadcasted_iota(jnp.int32, (keep.shape[1], lanes), 1)
    for r, out in enumerate(outs):
        total = keep[r] + got[r].astype(jnp.float32)
        out[:, :width] = total[:, :width].astype(out.dtype)
        value = jnp.sum(total[:, width:], axis=1, keepdims=True)
        out[:, width:] = thirds(jnp.broadcast_to(value, lane.shape), lane).astype(out.dtype)


def chip_sum(keep, got):
    depth, rows, width = keep.shape
    return pl.pallas_call(
        chip_sum_kernel,
        out_shape=[jax.ShapeDtypeStruct((rows, width), jnp.bfloat16)] * depth,
        name="chip_sum",
        compiler_params=pltpu.CompilerParams(vmem_limit_bytes=limit(6 * 2**20)),
    )(keep, got)


def chunk_sum_kernel(own, got, stats, chunk, loss):
    width = chunk.shape[1]
    total = own[...] + got[...]
    chunk[...] = total[:, :width].astype(chunk.dtype)
    value = jnp.sum(total[:8, width:], axis=1, keepdims=True)
    loss[...] = stats[1] * jnp.broadcast_to(value, loss.shape)


def chunk_sum(own, got, stats):
    rows, width = own.shape
    return pl.pallas_call(
        chunk_sum_kernel,
        in_specs=[vmem] * 3,
        out_specs=[vmem] * 2,
        out_shape=[
            jax.ShapeDtypeStruct((rows, width - lanes), jnp.bfloat16),
            jax.ShapeDtypeStruct((8, lanes), jnp.float32),
        ],
        name="chunk_sum",
        compiler_params=pltpu.CompilerParams(vmem_limit_bytes=limit(16 * rows * width)),
    )(own, got, stats)


def last_sum_kernel(own, near, far, stats, out):
    total = (own[...] + near[...].astype(jnp.float32)) + far[...].astype(jnp.float32)
    out[0] = stats[1][:1] * total


def last_sum(own, near, far, stats):
    rows, rank = own.shape
    return pl.pallas_call(
        last_sum_kernel,
        in_specs=[vmem] * 4,
        out_specs=vmem,
        out_shape=jax.ShapeDtypeStruct((1, rows, rank), jnp.float32),
        name="last_sum",
        compiler_params=pltpu.CompilerParams(vmem_limit_bytes=limit(16 * rows * rank)),
    )(own, near, far, stats)


def fill_kernel(own, other, out):
    depth, rows = own.shape[:2]
    z, _, k = place()
    for dk, source in enumerate((own, other)):
        for r in range(depth):
            at = (lax.bitwise_xor(z, r) * 2 + lax.bitwise_xor(k, dk)) * rows
            out[pl.ds(pl.multiple_of(at, rows), rows), :] = source[r].astype(jnp.float32)


def fill(own, other):
    depth, rows, width = own.shape
    return pl.pallas_call(
        fill_kernel,
        out_shape=jax.ShapeDtypeStruct((2 * depth * rows, width), jnp.float32),
        name="fill",
        compiler_params=pltpu.CompilerParams(vmem_limit_bytes=limit(6 * 2**20)),
    )(own, other)


def placed(activations, output_gradient, adapter_a, adapter_b, log_ratio, lengths, rewards):
    size = lax.axis_size("dp")
    depth = size // (2 * cores)
    rows, _ = adapter_a.shape[1:]
    everyone = [(zz, yy, kk) for zz in range(depth) for yy in range(2) for kk in range(cores)]
    number = lambda zz, yy, kk: (zz * 2 + yy) * cores + kk
    f32 = lambda value: value.astype(jnp.float32)
    half_width = lambda value: value.astype(jnp.bfloat16)

    def move(value, target):
        pairs = [(number(*at), number(*target(*at))) for at in everyone]
        return lax.ppermute(value, "dp", pairs)

    to_core = lambda value: move(value, lambda zz, yy, kk: (zz, yy, kk ^ 1))
    to_y = lambda value: move(value, lambda zz, yy, kk: (zz, yy ^ 1, kk))
    to_z = lambda value, r: move(value, lambda zz, yy, kk: (zz ^ r, yy, kk))
    across = lambda value, r: move(value, lambda zz, yy, kk: (zz ^ r, kk, yy))

    def other_tensor(value):
        return lax.ppermute(value, "tensor", [(0, 1), (1, 0)])

    first = lead()

    bit = depth // 2
    have = {0: adapter_a[0]}
    while bit:
        for r in sorted(have):
            have[r ^ bit] = to_z(have[r], bit)
        bit //= 2
    slices = []
    for r in range(depth):
        over = to_y(have[r])
        slices.append([have[r], to_core(have[r]), over, to_core(over)])

    back = back_part(output_gradient, adapter_b, first)
    coefficient, stats = terms(log_ratio, lengths, rewards)
    other_back = other_tensor(back)

    order = [r for r in range(depth - 1, -1, -1)]
    sums = {}
    pieces = grad_a_part(activations, coefficient, back, other_back, order, rows)
    for start in range(0, depth, 2):
        keep, send = pieces[start : start + 2]
        got = to_core(send)
        for index in range(2):
            sums[order[start + index]] = f32(keep[index]) + f32(got[index])
    got = to_y(half_width(jnp.stack([sums[1][1], sums[0][1]])))
    near = half_width(sums.pop(1)[0] + f32(got[0]))
    own = sums.pop(0)[0] + f32(got[1])
    bit = 1
    while 2 * bit < depth:
        for r in order:
            if r & bit and r in sums:
                got = to_z(half_width(sums.pop(r)), bit)
                sums[r ^ bit] = sums[r ^ bit] + f32(got)
        bit *= 2
    for r in list(sums):
        got = to_y(half_width(sums[r][1]))
        sums[r] = sums[r][0] + f32(got)
    near = to_z(near, 1)
    last = to_z(half_width(sums[bit]), bit)
    grad_a = last_sum(own, near, last, stats)

    cut = depth - 1
    low, _ = low_rank_part(activations, list(range(cut)), sum(slices[:cut], []))
    low, low_sent = low_rank_part(activations, list(range(cut, depth)), sum(slices[cut:], []), low)
    other = other_tensor(low_sent)
    keep, send = grad_b_part(low, other, coefficient, stats, output_gradient, depth)
    got = to_core(send)
    pieces = chip_sum(keep, got)
    total = 0.0
    for r in range(depth):
        total = total + f32(across(pieces[r], r))
    got = to_core(total)
    chunk, loss = chunk_sum(total, got, stats)
    own = jnp.stack([across(chunk, r) for r in range(depth)])
    grad_b = fill(own, to_core(own))
    return (grad_a, grad_b, loss[0, 0])


def local(*args):
    _, _, adapter_a = args[:3]
    size = lax.axis_size("dp")
    depth = size // (2 * cores)
    rows, rank = adapter_a.shape[1:]
    fits = (
        lax.axis_size("tensor") == 2
        and size == 2 * cores * depth
        and depth == 4
        and rows % 16 == 0
        and 4 * rows % lanes == 0
        and rank == lanes
        and rank % (32 * depth) == 0
        and args[4].shape[0] % lanes == 0
    )
    return placed(*args) if fits else general(*args)


def solution(mesh):
    in_specs = (
        P("dp", "tensor"),
        P("dp", "tensor"),
        P("tensor", "dp", None),
        P(None, "tensor"),
        P("dp"),
        P(),
        P(),
    )
    out_specs = (P("tensor", "dp", None), P(None, "tensor"), P())

    return jax.shard_map(local, mesh=mesh, in_specs=in_specs, out_specs=out_specs, check_vma=False)
```

```python
import functools

import jax
import jax.numpy as jnp
from jax import lax
from jax.experimental import pallas as pl
from jax.experimental.pallas import tpu as pltpu
from jax.sharding import PartitionSpec as P


clip_eps = 0.2
adapter_scale_factor = 2.0
cores = 2
lanes = 128


def slot_terms(length_row, reward_row, log_ratio, offset):
    reward = reward_row.astype(jnp.float32)
    center = jnp.mean(reward)
    spread = jnp.mean((reward - center) * (reward - center))
    advantage = (reward - center) / jnp.sqrt(spread + 1.0)
    ends = jnp.cumsum(length_row)
    starts = ends - length_row
    slots = jnp.arange(log_ratio.shape[0], dtype=jnp.int32) + offset
    member = ((slots[None, :] >= starts[:, None]) & (slots[None, :] < ends[:, None])).astype(
        jnp.float32
    )
    live = jnp.sum(member, axis=0)
    token_adv = jnp.sum(member * advantage[:, None], axis=0)
    ratio = jnp.exp(log_ratio)
    unclipped = ratio * token_adv
    clipped = jnp.clip(ratio, 1.0 - clip_eps, 1.0 + clip_eps) * token_adv
    token_loss = -jnp.minimum(unclipped, clipped)
    slope = jnp.where(unclipped <= clipped, -unclipped, jnp.zeros_like(unclipped))
    return (live * slope, jnp.sum(live * token_loss))


def own_terms(log_ratio, lengths, rewards):
    tokens = log_ratio.shape[0]
    groups = lengths.shape[0]
    per_group = lax.axis_size("dp") // groups
    position = lax.axis_index("dp")
    group_id = position // per_group
    offset = position % per_group * tokens
    length_row = lax.dynamic_index_in_dim(lengths, group_id, 0, keepdims=False)
    reward_row = lax.dynamic_index_in_dim(rewards, group_id, 0, keepdims=False)
    coefficient, loss = slot_terms(length_row, reward_row, log_ratio, offset)
    live = jnp.sum(jnp.minimum(jnp.sum(lengths, axis=1), per_group * tokens))
    return coefficient, loss, groups / live.astype(jnp.float32)


def general(activations, output_gradient, adapter_a, adapter_b, log_ratio, lengths, rewards):
    coefficient, loss, factor = own_terms(log_ratio, lengths, rewards)
    partial_low = jnp.dot(
        activations,
        lax.all_gather(adapter_a, "dp", axis=1, tiled=True)[0],
        preferred_element_type=jnp.float32,
    )
    partial_back = lax.dot_general(
        output_gradient, adapter_b, (((1,), (1,)), ((), ())), preferred_element_type=jnp.float32
    )
    low_rank, back = lax.psum((partial_low, partial_back), "tensor")
    error_rows = (adapter_scale_factor * coefficient[:, None] * back).astype(jnp.bfloat16)
    grad_b = adapter_scale_factor * jnp.einsum(
        "tr,td->rd",
        coefficient[:, None] * low_rank,
        output_gradient.astype(jnp.float32),
        precision=lax.Precision.HIGHEST,
    )
    grad_a = lax.psum_scatter(
        lax.dot_general(
            activations, error_rows, (((0,), (0,)), ((), ())), preferred_element_type=jnp.float32
        ),
        "dp",
        scatter_dimension=0,
        tiled=True,
    )
    grad_b, loss = lax.psum((grad_b, loss), "dp")
    return ((factor * grad_a)[None], factor * grad_b, factor * loss)


vmem = pl.BlockSpec(memory_space=pltpu.VMEM)


def limit(size):
    return size + 4 * 2**20


def place():
    position = lax.axis_index("dp")
    return position // (2 * cores), position // cores % 2, position % cores


def segment(dy, dk, rows):
    _, y, k = place()
    return pl.ds(pl.multiple_of((lax.bitwise_xor(y, dy) * 2 + lax.bitwise_xor(k, dk)) * rows, 16), rows)


def terms_kernel(lengths, rewards, log_ratio, spread_out, stats, *, per_group):
    groups, count = lengths.shape
    lines = log_ratio.shape[0]
    shape = (lines, lanes)
    tokens = lines * lanes
    position = lax.axis_index("dp")
    group = position // per_group
    value = [jnp.full(shape, rewards[group, i], jnp.int32).astype(jnp.float32) for i in range(count)]
    center = sum(value) / count
    spread = sum((v - center) * (v - center) for v in value) / count
    root = jnp.sqrt(spread + 1.0)
    slots = (
        lax.broadcasted_iota(jnp.int32, shape, 0) * lanes
        + lax.broadcasted_iota(jnp.int32, shape, 1)
        + position % per_group * tokens
    )
    token_adv = jnp.zeros(shape, jnp.float32)
    live = jnp.zeros(shape, jnp.float32)
    start = 0
    for i in range(count):
        end = start + lengths[group, i]
        member = ((slots >= start) & (slots < end)).astype(jnp.float32)
        token_adv = token_adv + member * ((value[i] - center) / root)
        live = live + member
        start = end
    ratio = jnp.exp(log_ratio[...])
    unclipped = ratio * token_adv
    clipped = jnp.clip(ratio, 1.0 - clip_eps, 1.0 + clip_eps) * token_adv
    loss = jnp.sum(live * -jnp.minimum(unclipped, clipped))
    coefficient = live * jnp.where(unclipped <= clipped, -unclipped, jnp.zeros(shape, jnp.float32))
    for line in range(lines):
        row = jnp.broadcast_to(coefficient[line : line + 1, :], (lanes, lanes))
        spread_out[line * lanes : (line + 1) * lanes, :] = row.T
    total = 0
    for g in range(groups):
        size = 0
        for i in range(count):
            size = size + lengths[g, i]
        total = total + jnp.minimum(size, per_group * tokens)
    stats[0] = jnp.broadcast_to(loss, stats.shape[1:])
    stats[1] = groups / jnp.full(stats.shape[1:], total, jnp.int32).astype(jnp.float32)


def terms(log_ratio, lengths, rewards):
    tokens = log_ratio.shape[0]
    per_group = lax.axis_size("dp") // lengths.shape[0]
    return pl.pallas_call(
        functools.partial(terms_kernel, per_group=per_group),
        in_specs=[pl.BlockSpec(memory_space=pltpu.SMEM)] * 2
        + [vmem],
        out_specs=[vmem] * 2,
        out_shape=[
            jax.ShapeDtypeStruct((tokens, lanes), jnp.float32),
            jax.ShapeDtypeStruct((2, 8, lanes), jnp.float32),
        ],
        name="terms",
        compiler_params=pltpu.CompilerParams(vmem_limit_bytes=limit(2**20)),
    )(lengths, rewards, log_ratio.reshape(tokens // lanes, lanes))


def lead_kernel(out):
    out[...] = jnp.zeros(out.shape, out.dtype)


def lead():
    return pl.pallas_call(
        lead_kernel,
        out_specs=vmem,
        out_shape=jax.ShapeDtypeStruct((8, lanes), jnp.float32),
        cost_estimate=pl.CostEstimate(flops=10**10, bytes_accessed=0, transcendentals=0),
        name="lead",
        compiler_params=pltpu.CompilerParams(vmem_limit_bytes=limit(0)),
    )()


def back_kernel(grad, factor, _, out):
    out[...] = lax.dot_general(
        grad[...], factor[...], (((1,), (1,)), ((), ())), preferred_element_type=jnp.float32
    )


def back_part(grad, factor, first):
    tokens, width = grad.shape
    rank = factor.shape[0]
    return pl.pallas_call(
        back_kernel,
        in_specs=[vmem] * 3,
        out_specs=vmem,
        out_shape=jax.ShapeDtypeStruct((tokens, rank), jnp.float32),
        cost_estimate=pl.CostEstimate(
            flops=2 * tokens * width * rank,
            bytes_accessed=2 * (tokens + rank) * width,
            transcendentals=0,
        ),
        name="back",
        compiler_params=pltpu.CompilerParams(
            vmem_limit_bytes=limit(2 * (tokens + rank) * width)
        ),
    )(grad, factor, first)


def tile_of(width):
    blocks = width // lanes
    return next(blocks // n for n in range(3, blocks + 1) if blocks % n == 0) * lanes


def columns(r, t, width, tile):
    at = lax.bitwise_xor(place()[0], r) * width + t * tile
    return pl.ds(pl.multiple_of(at, lanes), tile)


def low_rank_kernel(rounds, chained, acts, *refs):
    count = len(rounds)
    slices = refs[: 4 * count]
    outs, whole = refs[4 * count + chained : -1], refs[-1]
    rows = slices[0].shape[0]
    width = 4 * rows
    tile = tile_of(width)
    total = refs[4 * count][...] if chained else None
    for index, r in enumerate(rounds):
        for dy in range(2):
            for dk in range(2):
                whole[index, segment(dy, dk, rows)] = slices[4 * index + 2 * dy + dk][...]
        for t in range(width // tile):
            part = jnp.dot(
                acts[:, columns(r, t, width, tile)],
                whole[index, t * tile : (t + 1) * tile, :],
                preferred_element_type=jnp.float32,
            )
            total = part if total is None else total + part
    for out in outs:
        out[...] = total.astype(out.dtype)


def low_rank_part(activations, rounds, slices, kinds, before=None):
    tokens = activations.shape[0]
    rows, rank = slices[0].shape
    width = 4 * rows
    count = len(rounds)
    extra = () if before is None else (before,)
    return pl.pallas_call(
        functools.partial(low_rank_kernel, rounds, before is not None),
        in_specs=[vmem] * (1 + len(slices) + len(extra)),
        out_specs=[vmem] * len(kinds),
        scratch_shapes=[pltpu.VMEM((count, width, rank), jnp.bfloat16)],
        out_shape=[jax.ShapeDtypeStruct((tokens, rank), kind) for kind in kinds],
        cost_estimate=pl.CostEstimate(
            flops=2 * tokens * width * rank * count,
            bytes_accessed=2 * (tokens + rank) * width * count,
            transcendentals=0,
        ),
        name="low_rank",
        compiler_params=pltpu.CompilerParams(
            vmem_limit_bytes=limit(2 * activations.size + 4 * count * width * rank)
        ),
    )(activations, *slices, *extra)


def grad_a_kernel(order, acts, coefficient, back, other, *refs):
    outs, whole = refs[:-1], refs[-1]
    rows = outs[0].shape[2]
    width = 4 * rows
    tile = tile_of(width)
    scaled = adapter_scale_factor * coefficient[...] * (back[...] + other[...])
    err = scaled.astype(jnp.bfloat16)
    for index, r in enumerate(order):
        for t in range(width // tile):
            part = lax.dot_general(
                acts[:, columns(r, t, width, tile)],
                err,
                (((0,), (0,)), ((), ())),
                preferred_element_type=jnp.float32,
            )
            whole[index % 2, t * tile : (t + 1) * tile, :] = part.astype(jnp.bfloat16)
        for dk in range(2):
            for dy in range(2):
                outs[index // 2 * 2 + dk][index % 2, dy] = whole[
                    index % 2, segment(dy, dk, rows)
                ]


def grad_a_part(activations, coefficient, back, other, order, rows):
    tokens, rank = back.shape
    width = 4 * rows
    count = len(order)
    shape = jax.ShapeDtypeStruct((2, 2, rows, rank), jnp.bfloat16)
    return pl.pallas_call(
        functools.partial(grad_a_kernel, order),
        in_specs=[vmem] * 4,
        out_specs=[vmem] * count,
        scratch_shapes=[pltpu.VMEM((2, width, rank), jnp.bfloat16)],
        out_shape=[shape] * count,
        cost_estimate=pl.CostEstimate(
            flops=2 * tokens * width * rank * count,
            bytes_accessed=2 * (tokens + rank) * width * count,
            transcendentals=0,
        ),
        name="grad_a",
        compiler_params=pltpu.CompilerParams(
            vmem_limit_bytes=limit(2 * activations.size + 4 * count * width * rank)
        ),
    )(activations, coefficient, back, other)


def grad_b_kernel(low, other, coefficient, stats, grad, keep, send, whole):
    depth, rows = keep.shape[:2]
    width = grad.shape[1]
    tile = tile_of(width)
    scale = adapter_scale_factor * stats[1][:1] * coefficient[...]
    weighted = (scale * (low[...] + other[...].astype(jnp.float32))).astype(jnp.bfloat16)
    shape = (rows, lanes)
    parts = thirds(
        jnp.broadcast_to(stats[0][:1], shape), lax.broadcasted_iota(jnp.int32, shape, 1)
    )
    for t in range(width // tile):
        whole[:, t * tile : (t + 1) * tile] = lax.dot_general(
            weighted,
            grad[:, t * tile : (t + 1) * tile],
            (((0,), (0,)), ((), ())),
            preferred_element_type=jnp.float32,
        )
    z, _, k = place()
    for dk, out in enumerate((keep, send)):
        for r in range(depth):
            at = (lax.bitwise_xor(z, r) * 2 + lax.bitwise_xor(k, dk)) * rows
            out[r, :, :width] = whole[pl.ds(pl.multiple_of(at, rows), rows), :].astype(out.dtype)
            out[r, :, width:] = parts.astype(out.dtype)


def grad_b_part(low, other, coefficient, stats, grad, depth):
    tokens, rank = low.shape
    width = grad.shape[1]
    rows = rank // (2 * depth)
    shape = (depth, rows, width + lanes)
    return pl.pallas_call(
        grad_b_kernel,
        in_specs=[vmem] * 5,
        out_specs=[vmem] * 2,
        out_shape=[
            jax.ShapeDtypeStruct(shape, jnp.float32),
            jax.ShapeDtypeStruct(shape, jnp.bfloat16),
        ],
        scratch_shapes=[pltpu.VMEM((rank, width), jnp.float32)],
        cost_estimate=pl.CostEstimate(
            flops=2 * tokens * width * rank,
            bytes_accessed=2 * tokens * width + 6 * rank * width,
            transcendentals=0,
        ),
        name="grad_b",
        compiler_params=pltpu.CompilerParams(vmem_limit_bytes=limit(10 * rank * width)),
    )(low, other, coefficient, stats, grad)


def thirds(value, lane):
    high = value.astype(jnp.bfloat16).astype(jnp.float32)
    middle = (value - high).astype(jnp.bfloat16).astype(jnp.float32)
    low = value - high - middle
    zero = jnp.zeros_like(value)
    return jnp.where(
        lane == 0, high, jnp.where(lane == 1, middle, jnp.where(lane == 2, low, zero))
    )


def chip_sum_kernel(keep, got, *outs):
    width = keep.shape[2] - lanes
    lane = lax.broadcasted_iota(jnp.int32, (keep.shape[1], lanes), 1)
    for r, out in enumerate(outs):
        total = keep[r] + got[r].astype(jnp.float32)
        out[:, :width] = total[:, :width].astype(out.dtype)
        value = jnp.sum(total[:, width:], axis=1, keepdims=True)
        out[:, width:] = thirds(jnp.broadcast_to(value, lane.shape), lane).astype(out.dtype)


def chip_sum(keep, got):
    depth, rows, width = keep.shape
    return pl.pallas_call(
        chip_sum_kernel,
        out_shape=[jax.ShapeDtypeStruct((rows, width), jnp.bfloat16)] * depth,
        name="chip_sum",
        compiler_params=pltpu.CompilerParams(vmem_limit_bytes=limit(6 * 2**20)),
    )(keep, got)


def chunk_sum_kernel(own, got, stats, chunk, loss):
    width = chunk.shape[1]
    total = own[...] + got[...]
    chunk[...] = total[:, :width].astype(chunk.dtype)
    value = jnp.sum(total[:8, width:], axis=1, keepdims=True)
    loss[...] = stats[1] * jnp.broadcast_to(value, loss.shape)


def chunk_sum(own, got, stats):
    rows, width = own.shape
    return pl.pallas_call(
        chunk_sum_kernel,
        in_specs=[vmem] * 3,
        out_specs=[vmem] * 2,
        out_shape=[
            jax.ShapeDtypeStruct((rows, width - lanes), jnp.bfloat16),
            jax.ShapeDtypeStruct((8, lanes), jnp.float32),
        ],
        name="chunk_sum",
        compiler_params=pltpu.CompilerParams(vmem_limit_bytes=limit(16 * rows * width)),
    )(own, got, stats)


def last_sum_kernel(own, near, far, stats, out):
    total = (own[...] + near[...].astype(jnp.float32)) + far[...].astype(jnp.float32)
    out[0] = stats[1][:1] * total


def last_sum(own, near, far, stats):
    rows, rank = own.shape
    return pl.pallas_call(
        last_sum_kernel,
        in_specs=[vmem] * 4,
        out_specs=vmem,
        out_shape=jax.ShapeDtypeStruct((1, rows, rank), jnp.float32),
        name="last_sum",
        compiler_params=pltpu.CompilerParams(vmem_limit_bytes=limit(16 * rows * rank)),
    )(own, near, far, stats)


def fill_kernel(own, other, out):
    depth, rows = own.shape[:2]
    z, _, k = place()
    for dk, source in enumerate((own, other)):
        for r in range(depth):
            at = (lax.bitwise_xor(z, r) * 2 + lax.bitwise_xor(k, dk)) * rows
            out[pl.ds(pl.multiple_of(at, rows), rows), :] = source[r].astype(jnp.float32)


def fill(own, other):
    depth, rows, width = own.shape
    return pl.pallas_call(
        fill_kernel,
        out_shape=jax.ShapeDtypeStruct((2 * depth * rows, width), jnp.float32),
        name="fill",
        compiler_params=pltpu.CompilerParams(vmem_limit_bytes=limit(6 * 2**20)),
    )(own, other)


def placed(activations, output_gradient, adapter_a, adapter_b, log_ratio, lengths, rewards):
    size = lax.axis_size("dp")
    depth = size // (2 * cores)
    rows, _ = adapter_a.shape[1:]
    everyone = [(zz, yy, kk) for zz in range(depth) for yy in range(2) for kk in range(cores)]
    number = lambda zz, yy, kk: (zz * 2 + yy) * cores + kk
    f32 = lambda value: value.astype(jnp.float32)
    half_width = lambda value: value.astype(jnp.bfloat16)

    def move(value, target):
        pairs = [(number(*at), number(*target(*at))) for at in everyone]
        return lax.ppermute(value, "dp", pairs)

    to_core = lambda value: move(value, lambda zz, yy, kk: (zz, yy, kk ^ 1))
    to_y = lambda value: move(value, lambda zz, yy, kk: (zz, yy ^ 1, kk))
    to_z = lambda value, r: move(value, lambda zz, yy, kk: (zz ^ r, yy, kk))
    across = lambda value, r: move(value, lambda zz, yy, kk: (zz ^ r, kk, yy))

    def other_tensor(value):
        return lax.ppermute(value, "tensor", [(0, 1), (1, 0)])

    first = lead()

    bit = depth // 2
    have = {0: adapter_a[0]}
    while bit:
        for r in sorted(have):
            have[r ^ bit] = to_z(have[r], bit)
        bit //= 2
    slices = []
    for r in range(depth):
        over = to_y(have[r])
        slices.append([have[r], to_core(have[r]), over, to_core(over)])

    back = back_part(output_gradient, adapter_b, first)
    coefficient, stats = terms(log_ratio, lengths, rewards)
    other_back = other_tensor(back)

    order = [r for r in range(depth - 1, -1, -1)]
    sums = {}
    pieces = grad_a_part(activations, coefficient, back, other_back, order, rows)
    for start in range(0, depth, 2):
        keep, send = pieces[start : start + 2]
        got = to_core(send)
        for index in range(2):
            sums[order[start + index]] = f32(keep[index]) + f32(got[index])
    got = to_y(half_width(jnp.stack([sums[1][1], sums[0][1]])))
    near = half_width(sums.pop(1)[0] + f32(got[0]))
    own = sums.pop(0)[0] + f32(got[1])
    bit = 1
    while 2 * bit < depth:
        for r in order:
            if r & bit and r in sums:
                got = to_z(half_width(sums.pop(r)), bit)
                sums[r ^ bit] = sums[r ^ bit] + f32(got)
        bit *= 2
    for r in list(sums):
        got = to_y(half_width(sums[r][1]))
        sums[r] = sums[r][0] + f32(got)
    near = to_z(near, 1)
    last = to_z(half_width(sums[bit]), bit)
    grad_a = last_sum(own, near, last, stats)

    cut = depth - 1
    (low,) = low_rank_part(
        activations, list(range(cut)), sum(slices[:cut], []), [jnp.float32]
    )
    low, low_sent = low_rank_part(
        activations,
        list(range(cut, depth)),
        sum(slices[cut:], []),
        [jnp.float32, jnp.bfloat16],
        low,
    )
    other = other_tensor(low_sent)
    keep, send = grad_b_part(low, other, coefficient, stats, output_gradient, depth)
    got = to_core(send)
    pieces = chip_sum(keep, got)
    total = 0.0
    for r in range(depth):
        total = total + f32(across(pieces[r], r))
    got = to_core(total)
    chunk, loss = chunk_sum(total, got, stats)
    own = jnp.stack([across(chunk, r) for r in range(depth)])
    grad_b = fill(own, to_core(own))
    return (grad_a, grad_b, loss[0, 0])


def local(*args):
    _, _, adapter_a = args[:3]
    size = lax.axis_size("dp")
    depth = size // (2 * cores)
    rows, rank = adapter_a.shape[1:]
    fits = (
        lax.axis_size("tensor") == 2
        and size == 2 * cores * depth
        and depth == 4
        and rows % 16 == 0
        and 4 * rows % lanes == 0
        and rank == lanes
        and rank % (32 * depth) == 0
        and args[4].shape[0] % lanes == 0
    )
    return placed(*args) if fits else general(*args)


def solution(mesh):
    in_specs = (
        P("dp", "tensor"),
        P("dp", "tensor"),
        P("tensor", "dp", None),
        P(None, "tensor"),
        P("dp"),
        P(),
        P(),
    )
    out_specs = (P("tensor", "dp", None), P(None, "tensor"), P())

    return jax.shard_map(local, mesh=mesh, in_specs=in_specs, out_specs=out_specs, check_vma=False)
```

```python
import functools

import jax
import jax.numpy as jnp
from jax import lax
from jax.experimental import pallas as pl
from jax.experimental.pallas import tpu as pltpu
from jax.sharding import PartitionSpec as P


clip_eps = 0.2
adapter_scale_factor = 2.0
cores = 2
lanes = 128


def slot_terms(length_row, reward_row, log_ratio, offset):
    reward = reward_row.astype(jnp.float32)
    center = jnp.mean(reward)
    spread = jnp.mean((reward - center) * (reward - center))
    advantage = (reward - center) / jnp.sqrt(spread + 1.0)
    ends = jnp.cumsum(length_row)
    starts = ends - length_row
    slots = jnp.arange(log_ratio.shape[0], dtype=jnp.int32) + offset
    member = ((slots[None, :] >= starts[:, None]) & (slots[None, :] < ends[:, None])).astype(
        jnp.float32
    )
    live = jnp.sum(member, axis=0)
    token_adv = jnp.sum(member * advantage[:, None], axis=0)
    ratio = jnp.exp(log_ratio)
    unclipped = ratio * token_adv
    clipped = jnp.clip(ratio, 1.0 - clip_eps, 1.0 + clip_eps) * token_adv
    token_loss = -jnp.minimum(unclipped, clipped)
    slope = jnp.where(unclipped <= clipped, -unclipped, jnp.zeros_like(unclipped))
    return (live * slope, jnp.sum(live * token_loss))


def own_terms(log_ratio, lengths, rewards):
    tokens = log_ratio.shape[0]
    groups = lengths.shape[0]
    per_group = lax.axis_size("dp") // groups
    position = lax.axis_index("dp")
    group_id = position // per_group
    offset = position % per_group * tokens
    length_row = lax.dynamic_index_in_dim(lengths, group_id, 0, keepdims=False)
    reward_row = lax.dynamic_index_in_dim(rewards, group_id, 0, keepdims=False)
    coefficient, loss = slot_terms(length_row, reward_row, log_ratio, offset)
    live = jnp.sum(jnp.minimum(jnp.sum(lengths, axis=1), per_group * tokens))
    return coefficient, loss, groups / live.astype(jnp.float32)


def general(activations, output_gradient, adapter_a, adapter_b, log_ratio, lengths, rewards):
    coefficient, loss, factor = own_terms(log_ratio, lengths, rewards)
    partial_low = jnp.dot(
        activations,
        lax.all_gather(adapter_a, "dp", axis=1, tiled=True)[0],
        preferred_element_type=jnp.float32,
    )
    partial_back = lax.dot_general(
        output_gradient, adapter_b, (((1,), (1,)), ((), ())), preferred_element_type=jnp.float32
    )
    low_rank, back = lax.psum((partial_low, partial_back), "tensor")
    error_rows = (adapter_scale_factor * coefficient[:, None] * back).astype(jnp.bfloat16)
    grad_b = adapter_scale_factor * jnp.einsum(
        "tr,td->rd",
        coefficient[:, None] * low_rank,
        output_gradient.astype(jnp.float32),
        precision=lax.Precision.HIGHEST,
    )
    grad_a = lax.psum_scatter(
        lax.dot_general(
            activations, error_rows, (((0,), (0,)), ((), ())), preferred_element_type=jnp.float32
        ),
        "dp",
        scatter_dimension=0,
        tiled=True,
    )
    grad_b, loss = lax.psum((grad_b, loss), "dp")
    return ((factor * grad_a)[None], factor * grad_b, factor * loss)


vmem = pl.BlockSpec(memory_space=pltpu.VMEM)


def limit(size):
    return size + 4 * 2**20


def place():
    position = lax.axis_index("dp")
    return position // (2 * cores), position // cores % 2, position % cores


def segment(dy, dk, rows):
    _, y, k = place()
    return pl.ds(pl.multiple_of((lax.bitwise_xor(y, dy) * 2 + lax.bitwise_xor(k, dk)) * rows, 16), rows)


def terms_kernel(lengths, rewards, log_ratio, spread_out, stats, *, per_group):
    groups, count = lengths.shape
    lines = log_ratio.shape[0]
    shape = (lines, lanes)
    tokens = lines * lanes
    position = lax.axis_index("dp")
    group = position // per_group
    value = [jnp.full(shape, rewards[group, i], jnp.int32).astype(jnp.float32) for i in range(count)]
    center = sum(value) / count
    spread = sum((v - center) * (v - center) for v in value) / count
    root = jnp.sqrt(spread + 1.0)
    slots = (
        lax.broadcasted_iota(jnp.int32, shape, 0) * lanes
        + lax.broadcasted_iota(jnp.int32, shape, 1)
        + position % per_group * tokens
    )
    token_adv = jnp.zeros(shape, jnp.float32)
    live = jnp.zeros(shape, jnp.float32)
    start = 0
    for i in range(count):
        end = start + lengths[group, i]
        member = ((slots >= start) & (slots < end)).astype(jnp.float32)
        token_adv = token_adv + member * ((value[i] - center) / root)
        live = live + member
        start = end
    ratio = jnp.exp(log_ratio[...])
    unclipped = ratio * token_adv
    clipped = jnp.clip(ratio, 1.0 - clip_eps, 1.0 + clip_eps) * token_adv
    loss = jnp.sum(live * -jnp.minimum(unclipped, clipped))
    coefficient = live * jnp.where(unclipped <= clipped, -unclipped, jnp.zeros(shape, jnp.float32))
    for line in range(lines):
        row = jnp.broadcast_to(coefficient[line : line + 1, :], (lanes, lanes))
        spread_out[line * lanes : (line + 1) * lanes, :] = row.T
    total = 0
    for g in range(groups):
        size = 0
        for i in range(count):
            size = size + lengths[g, i]
        total = total + jnp.minimum(size, per_group * tokens)
    stats[0] = jnp.broadcast_to(loss, stats.shape[1:])
    stats[1] = groups / jnp.full(stats.shape[1:], total, jnp.int32).astype(jnp.float32)


def terms(log_ratio, lengths, rewards):
    tokens = log_ratio.shape[0]
    per_group = lax.axis_size("dp") // lengths.shape[0]
    return pl.pallas_call(
        functools.partial(terms_kernel, per_group=per_group),
        in_specs=[pl.BlockSpec(memory_space=pltpu.SMEM)] * 2
        + [vmem],
        out_specs=[vmem] * 2,
        out_shape=[
            jax.ShapeDtypeStruct((tokens, lanes), jnp.float32),
            jax.ShapeDtypeStruct((2, 8, lanes), jnp.float32),
        ],
        name="terms",
        compiler_params=pltpu.CompilerParams(vmem_limit_bytes=limit(2**20)),
    )(lengths, rewards, log_ratio.reshape(tokens // lanes, lanes))


def lead_kernel(out):
    out[...] = jnp.zeros(out.shape, out.dtype)


def lead():
    return pl.pallas_call(
        lead_kernel,
        out_specs=vmem,
        out_shape=jax.ShapeDtypeStruct((8, lanes), jnp.float32),
        cost_estimate=pl.CostEstimate(flops=10**10, bytes_accessed=0, transcendentals=0),
        name="lead",
        compiler_params=pltpu.CompilerParams(vmem_limit_bytes=limit(0)),
    )()


def back_kernel(grad, factor, _, out):
    out[...] = lax.dot_general(
        grad[...], factor[...], (((1,), (1,)), ((), ())), preferred_element_type=jnp.float32
    )


def back_part(grad, factor, first):
    tokens, width = grad.shape
    rank = factor.shape[0]
    return pl.pallas_call(
        back_kernel,
        in_specs=[vmem] * 3,
        out_specs=vmem,
        out_shape=jax.ShapeDtypeStruct((tokens, rank), jnp.float32),
        cost_estimate=pl.CostEstimate(
            flops=2 * tokens * width * rank,
            bytes_accessed=2 * (tokens + rank) * width,
            transcendentals=0,
        ),
        name="back",
        compiler_params=pltpu.CompilerParams(
            vmem_limit_bytes=limit(2 * (tokens + rank) * width)
        ),
    )(grad, factor, first)


def tile_of(width):
    blocks = width // lanes
    return next(blocks // n for n in range(3, blocks + 1) if blocks % n == 0) * lanes


def columns(r, t, width, tile):
    at = lax.bitwise_xor(place()[0], r) * width + t * tile
    return pl.ds(pl.multiple_of(at, lanes), tile)


def low_rank_kernel(rounds, chained, acts, *refs):
    count = len(rounds)
    slices = refs[: 4 * count]
    outs, whole = refs[4 * count + chained : -1], refs[-1]
    rows = slices[0].shape[0]
    width = 4 * rows
    tile = tile_of(width)
    total = refs[4 * count][...] if chained else None
    for index, r in enumerate(rounds):
        for dy in range(2):
            for dk in range(2):
                whole[index, segment(dy, dk, rows)] = slices[4 * index + 2 * dy + dk][...]
        for t in range(width // tile):
            part = jnp.dot(
                acts[:, columns(r, t, width, tile)],
                whole[index, t * tile : (t + 1) * tile, :],
                preferred_element_type=jnp.float32,
            )
            total = part if total is None else total + part
    for out in outs:
        out[...] = total.astype(out.dtype)


def low_rank_part(activations, rounds, slices, kinds, before=None):
    tokens = activations.shape[0]
    rows, rank = slices[0].shape
    width = 4 * rows
    count = len(rounds)
    extra = () if before is None else (before,)
    return pl.pallas_call(
        functools.partial(low_rank_kernel, rounds, before is not None),
        in_specs=[vmem] * (1 + len(slices) + len(extra)),
        out_specs=[vmem] * len(kinds),
        scratch_shapes=[pltpu.VMEM((count, width, rank), jnp.bfloat16)],
        out_shape=[jax.ShapeDtypeStruct((tokens, rank), kind) for kind in kinds],
        cost_estimate=pl.CostEstimate(
            flops=2 * tokens * width * rank * count,
            bytes_accessed=2 * (tokens + rank) * width * count,
            transcendentals=0,
        ),
        name="low_rank",
        compiler_params=pltpu.CompilerParams(
            vmem_limit_bytes=limit(2 * activations.size + 4 * count * width * rank)
        ),
    )(activations, *slices, *extra)


def grad_a_kernel(order, acts, coefficient, back, other, *refs):
    outs, whole = refs[:-1], refs[-1]
    rows = outs[0].shape[2]
    width = 4 * rows
    tile = tile_of(width)
    scaled = adapter_scale_factor * coefficient[...] * (back[...] + other[...])
    err = scaled.astype(jnp.bfloat16)
    for index, r in enumerate(order):
        for t in range(width // tile):
            part = lax.dot_general(
                acts[:, columns(r, t, width, tile)],
                err,
                (((0,), (0,)), ((), ())),
                preferred_element_type=jnp.float32,
            )
            whole[index % 2, t * tile : (t + 1) * tile, :] = part.astype(jnp.bfloat16)
        for dk in range(2):
            for dy in range(2):
                outs[index // 2 * 2 + dk][index % 2, dy] = whole[
                    index % 2, segment(dy, dk, rows)
                ]


def grad_a_part(activations, coefficient, back, other, order, rows):
    tokens, rank = back.shape
    width = 4 * rows
    count = len(order)
    shape = jax.ShapeDtypeStruct((2, 2, rows, rank), jnp.bfloat16)
    return pl.pallas_call(
        functools.partial(grad_a_kernel, order),
        in_specs=[vmem] * 4,
        out_specs=[vmem] * count,
        scratch_shapes=[pltpu.VMEM((2, width, rank), jnp.bfloat16)],
        out_shape=[shape] * count,
        cost_estimate=pl.CostEstimate(
            flops=2 * tokens * width * rank * count,
            bytes_accessed=2 * (tokens + rank) * width * count,
            transcendentals=0,
        ),
        name="grad_a",
        compiler_params=pltpu.CompilerParams(
            vmem_limit_bytes=limit(2 * activations.size + 4 * count * width * rank)
        ),
    )(activations, coefficient, back, other)


def grad_b_kernel(low, other, coefficient, stats, grad, keep, send, whole):
    depth, rows = keep.shape[:2]
    width = grad.shape[1]
    tile = tile_of(width)
    scale = adapter_scale_factor * stats[1][:1] * coefficient[...]
    weighted = (scale * (low[...] + other[...].astype(jnp.float32))).astype(jnp.bfloat16)
    shape = (rows, lanes)
    parts = thirds(
        jnp.broadcast_to(stats[0][:1], shape), lax.broadcasted_iota(jnp.int32, shape, 1)
    )
    for t in range(width // tile):
        whole[:, t * tile : (t + 1) * tile] = lax.dot_general(
            weighted,
            grad[:, t * tile : (t + 1) * tile],
            (((0,), (0,)), ((), ())),
            preferred_element_type=jnp.float32,
        )
    z, _, k = place()
    for dk, out in enumerate((keep, send)):
        for r in range(depth):
            at = (lax.bitwise_xor(z, r) * 2 + lax.bitwise_xor(k, dk)) * rows
            out[r, :, :width] = whole[pl.ds(pl.multiple_of(at, rows), rows), :].astype(out.dtype)
            out[r, :, width:] = parts.astype(out.dtype)


def grad_b_part(low, other, coefficient, stats, grad, depth):
    tokens, rank = low.shape
    width = grad.shape[1]
    rows = rank // (2 * depth)
    shape = (depth, rows, width + lanes)
    return pl.pallas_call(
        grad_b_kernel,
        in_specs=[vmem] * 5,
        out_specs=[vmem] * 2,
        out_shape=[
            jax.ShapeDtypeStruct(shape, jnp.float32),
            jax.ShapeDtypeStruct(shape, jnp.bfloat16),
        ],
        scratch_shapes=[pltpu.VMEM((rank, width), jnp.float32)],
        cost_estimate=pl.CostEstimate(
            flops=2 * tokens * width * rank,
            bytes_accessed=2 * tokens * width + 6 * rank * width,
            transcendentals=0,
        ),
        name="grad_b",
        compiler_params=pltpu.CompilerParams(vmem_limit_bytes=limit(10 * rank * width)),
    )(low, other, coefficient, stats, grad)


def thirds(value, lane):
    high = value.astype(jnp.bfloat16).astype(jnp.float32)
    middle = (value - high).astype(jnp.bfloat16).astype(jnp.float32)
    low = value - high - middle
    zero = jnp.zeros_like(value)
    return jnp.where(
        lane == 0, high, jnp.where(lane == 1, middle, jnp.where(lane == 2, low, zero))
    )


def chip_sum_kernel(keep, got, *outs):
    width = keep.shape[2] - lanes
    lane = lax.broadcasted_iota(jnp.int32, (keep.shape[1], lanes), 1)
    for r, out in enumerate(outs):
        total = keep[r] + got[r].astype(jnp.float32)
        out[:, :width] = total[:, :width].astype(out.dtype)
        value = jnp.sum(total[:, width:], axis=1, keepdims=True)
        out[:, width:] = thirds(jnp.broadcast_to(value, lane.shape), lane).astype(out.dtype)


def chip_sum(keep, got):
    depth, rows, width = keep.shape
    return pl.pallas_call(
        chip_sum_kernel,
        out_shape=[jax.ShapeDtypeStruct((rows, width), jnp.bfloat16)] * depth,
        name="chip_sum",
        compiler_params=pltpu.CompilerParams(vmem_limit_bytes=limit(6 * 2**20)),
    )(keep, got)


def chunk_sum_kernel(own, got, stats, chunk, loss):
    width = chunk.shape[1]
    total = own[...] + got[...]
    chunk[...] = total[:, :width].astype(chunk.dtype)
    value = jnp.sum(total[:8, width:], axis=1, keepdims=True)
    loss[...] = stats[1] * jnp.broadcast_to(value, loss.shape)


def chunk_sum(own, got, stats):
    rows, width = own.shape
    return pl.pallas_call(
        chunk_sum_kernel,
        in_specs=[vmem] * 3,
        out_specs=[vmem] * 2,
        out_shape=[
            jax.ShapeDtypeStruct((rows, width - lanes), jnp.bfloat16),
            jax.ShapeDtypeStruct((8, lanes), jnp.float32),
        ],
        name="chunk_sum",
        compiler_params=pltpu.CompilerParams(vmem_limit_bytes=limit(16 * rows * width)),
    )(own, got, stats)


def last_sum_kernel(own, near, far, stats, out):
    total = (own[...] + near[...].astype(jnp.float32)) + far[...].astype(jnp.float32)
    out[0] = stats[1][:1] * total


def last_sum(own, near, far, stats):
    rows, rank = own.shape
    return pl.pallas_call(
        last_sum_kernel,
        in_specs=[vmem] * 4,
        out_specs=vmem,
        out_shape=jax.ShapeDtypeStruct((1, rows, rank), jnp.float32),
        name="last_sum",
        compiler_params=pltpu.CompilerParams(vmem_limit_bytes=limit(16 * rows * rank)),
    )(own, near, far, stats)


def fill_kernel(dk, *refs):
    source, out, wide, sems = refs[0], *refs[-3:]
    depth, rows = source.shape[:2]
    z, _, k = place()
    copies = []
    for r in range(depth):
        wide[r] = source[r].astype(jnp.float32)
        at = (lax.bitwise_xor(z, r) * 2 + lax.bitwise_xor(k, dk)) * rows
        copy = pltpu.make_async_copy(
            wide.at[r], out.at[pl.ds(pl.multiple_of(at, rows), rows)], sems.at[r]
        )
        copy.start()
        copies.append(copy)
    for copy in copies:
        copy.wait()


def fill(dk, source, *before):
    depth, rows, width = source.shape
    anywhere = pl.BlockSpec(memory_space=pl.ANY)
    return pl.pallas_call(
        functools.partial(fill_kernel, dk),
        in_specs=[vmem] + [anywhere] * len(before),
        out_specs=anywhere,
        out_shape=jax.ShapeDtypeStruct((2 * depth * rows, width), jnp.float32),
        scratch_shapes=[
            pltpu.VMEM((depth, rows, width), jnp.float32),
            pltpu.SemaphoreType.DMA((depth,)),
        ],
        input_output_aliases={1: 0} if before else {},
        name="fill",
        compiler_params=pltpu.CompilerParams(
            vmem_limit_bytes=limit(8 * depth * rows * width)
        ),
    )(source, *before)


def placed(activations, output_gradient, adapter_a, adapter_b, log_ratio, lengths, rewards):
    size = lax.axis_size("dp")
    depth = size // (2 * cores)
    rows, _ = adapter_a.shape[1:]
    everyone = [(zz, yy, kk) for zz in range(depth) for yy in range(2) for kk in range(cores)]
    number = lambda zz, yy, kk: (zz * 2 + yy) * cores + kk
    f32 = lambda value: value.astype(jnp.float32)
    half_width = lambda value: value.astype(jnp.bfloat16)

    def move(value, target):
        pairs = [(number(*at), number(*target(*at))) for at in everyone]
        return lax.ppermute(value, "dp", pairs)

    to_core = lambda value: move(value, lambda zz, yy, kk: (zz, yy, kk ^ 1))
    to_y = lambda value: move(value, lambda zz, yy, kk: (zz, yy ^ 1, kk))
    to_z = lambda value, r: move(value, lambda zz, yy, kk: (zz ^ r, yy, kk))
    across = lambda value, r: move(value, lambda zz, yy, kk: (zz ^ r, kk, yy))

    def other_tensor(value):
        return lax.ppermute(value, "tensor", [(0, 1), (1, 0)])

    first = lead()

    bit = depth // 2
    have = {0: adapter_a[0]}
    while bit:
        for r in sorted(have):
            have[r ^ bit] = to_z(have[r], bit)
        bit //= 2
    slices = []
    for r in range(depth):
        over = to_y(have[r])
        slices.append([have[r], to_core(have[r]), over, to_core(over)])

    back = back_part(output_gradient, adapter_b, first)
    coefficient, stats = terms(log_ratio, lengths, rewards)
    other_back = other_tensor(back)

    order = [r for r in range(depth - 1, -1, -1)]
    sums = {}
    pieces = grad_a_part(activations, coefficient, back, other_back, order, rows)
    for start in range(0, depth, 2):
        keep, send = pieces[start : start + 2]
        got = to_core(send)
        for index in range(2):
            sums[order[start + index]] = f32(keep[index]) + f32(got[index])
    got = to_y(half_width(jnp.stack([sums[1][1], sums[0][1]])))
    near = half_width(sums.pop(1)[0] + f32(got[0]))
    own = sums.pop(0)[0] + f32(got[1])
    bit = 1
    while 2 * bit < depth:
        for r in order:
            if r & bit and r in sums:
                got = to_z(half_width(sums.pop(r)), bit)
                sums[r ^ bit] = sums[r ^ bit] + f32(got)
        bit *= 2
    for r in list(sums):
        got = to_y(half_width(sums[r][1]))
        sums[r] = sums[r][0] + f32(got)
    near = to_z(near, 1)
    last = to_z(half_width(sums[bit]), bit)
    grad_a = last_sum(own, near, last, stats)

    cut = depth - 1
    (low,) = low_rank_part(
        activations, list(range(cut)), sum(slices[:cut], []), [jnp.float32]
    )
    low, low_sent = low_rank_part(
        activations,
        list(range(cut, depth)),
        sum(slices[cut:], []),
        [jnp.float32, jnp.bfloat16],
        low,
    )
    other = other_tensor(low_sent)
    keep, send = grad_b_part(low, other, coefficient, stats, output_gradient, depth)
    got = to_core(send)
    pieces = chip_sum(keep, got)
    total = 0.0
    for r in range(depth):
        total = total + f32(across(pieces[r], r))
    got = to_core(total)
    chunk, loss = chunk_sum(total, got, stats)
    own = jnp.stack([across(chunk, r) for r in range(depth)])
    other = to_core(own)
    grad_b = fill(0, own)
    grad_b = fill(1, other, grad_b)
    return (grad_a, grad_b, loss[0, 0])


def local(*args):
    _, _, adapter_a = args[:3]
    size = lax.axis_size("dp")
    depth = size // (2 * cores)
    rows, rank = adapter_a.shape[1:]
    fits = (
        lax.axis_size("tensor") == 2
        and size == 2 * cores * depth
        and depth == 4
        and rows % 16 == 0
        and 4 * rows % lanes == 0
        and rank == lanes
        and rank % (32 * depth) == 0
        and args[4].shape[0] % lanes == 0
    )
    return placed(*args) if fits else general(*args)


def solution(mesh):
    in_specs = (
        P("dp", "tensor"),
        P("dp", "tensor"),
        P("tensor", "dp", None),
        P(None, "tensor"),
        P("dp"),
        P(),
        P(),
    )
    out_specs = (P("tensor", "dp", None), P(None, "tensor"), P())

    return jax.shard_map(local, mesh=mesh, in_specs=in_specs, out_specs=out_specs, check_vma=False)
```
